128 devices in a mesh: rows: 128 (over z, y, x, core).
Axes of the slice: x: 4, y: 4, z: 4, core: 2. Of those that a mesh axis runs over, the one named last changes fastest.
Arguments:
- events: float32 [4, 32, 1048576], P(None, None, 'rows'), may hold values from -8 to 8
- keep_indicator: int32 [4, 1048576], P(None, 'rows'), may hold values from 0 to 1, as said below
Outputs:
- lagging_mean: float32 [4, 32, 1048576], P(None, None, 'rows')
- deviation: float32 [4, 32, 1048576], P(None, None, 'rows')
The draws below stay inside these ranges and needn't reach their ends.
Inputs may be any that keep to these rules, and one draw needn't show every extreme that they name: `keep_indicator`: in each table, each of the 128 aligned blocks of 8192 rows holds at least 4096 survivors, and some block holds exactly 4096.
All inputs are finite; a program needn't handle non-finite values.
Results may differ from the reference program's by a relative error of at most 0.0003.
Values sent between devices are 32-bit elements; how exact they have to be, the bound alone decides.
No kernel may reach another device: no remote copies, remote signals or barrier semaphores. Data moves between devices by JAX's collectives and lax.ppermute only.
A program may use at most 128 MiB of HBM per device.

```python
import jax
import jax.numpy as jnp
from jax import lax

COLS = 32
SPAN_LENGTH = 4096
STREAMS = 4
ROWS_DEV = 8192
N_ROWS = 128


def draw_events(key, part):
    noise_key, level_key = jax.random.split(jax.random.fold_in(key, 11), 2)
    shape = (STREAMS, COLS, ROWS_DEV * N_ROWS)
    noise = jax.random.truncated_normal(noise_key, -4.0, 4.0, shape, jnp.float32)
    levels = jax.random.uniform(level_key, (STREAMS, 1, N_ROWS), jnp.float32, -2.0, 2.0)
    levels = jnp.broadcast_to(levels, (STREAMS, COLS, N_ROWS))
    spread = jnp.repeat(levels, ROWS_DEV, axis=2, total_repeat_length=ROWS_DEV * N_ROWS)
    return (noise + spread).astype(jnp.float32)


def draw_keep_indicator(key, part):
    count_key, perm_key, forced_key = jax.random.split(jax.random.fold_in(key, 23), 3)
    draws = jax.random.randint(count_key, (STREAMS, N_ROWS, 2), 0, ROWS_DEV - SPAN_LENGTH + 1)
    keep = SPAN_LENGTH + jnp.min(draws, axis=2)
    forced = jax.random.randint(forced_key, (STREAMS, 1), 0, N_ROWS)
    keep = jnp.where(jnp.arange(N_ROWS)[None, :] == forced, SPAN_LENGTH, keep)
    keys = jax.random.split(perm_key, STREAMS * N_ROWS)
    perms = jax.vmap(lambda single: jax.random.permutation(single, ROWS_DEV))(keys)
    perms = perms.reshape(STREAMS, N_ROWS, ROWS_DEV)
    mask = (perms < keep[:, :, None]).astype(jnp.int32)
    return mask.reshape(STREAMS, N_ROWS * ROWS_DEV)


def setup_inputs(seed: int = 0) -> dict:
    streams_of = jax.random.split(jax.random.key(seed), 3)
    return {
        "events": draw_events(jax.random.fold_in(streams_of[2], 71), 0),
        "keep_indicator": draw_keep_indicator(jax.random.fold_in(streams_of[2], 71), 0),
    }


def single_table_input(pair):
    values, persisting_flags = pair
    feature_width = values.shape[0]
    total_rows = values.shape[1]
    retained_rows = values * persisting_flags[None, :].astype(jnp.float32)
    order = jnp.argsort(1 - persisting_flags, stable=True).astype(jnp.int32)
    packed_entries = jnp.take(retained_rows, order, axis=1)
    extended = jnp.concatenate([jnp.zeros((feature_width, SPAN_LENGTH), jnp.float32), packed_entries], axis=1)
    blocks = extended.reshape(feature_width, (total_rows + SPAN_LENGTH) // SPAN_LENGTH, SPAN_LENGTH)
    partial_sums = jnp.cumsum(blocks, axis=2)
    whole = partial_sums[:, :, -1]
    trailing = partial_sums[:, 1:, :] + (whole[:, :-1, None] - partial_sums[:, :-1, :])
    trailing = trailing.reshape(feature_width, total_rows)
    remaining_position = jnp.cumsum(persisting_flags).astype(jnp.int32)
    gather_slot = jnp.maximum(remaining_position - 1, 0).astype(jnp.int32)
    selected_entries = jnp.take(trailing, gather_slot, axis=1)
    lagging_mean = jnp.where(remaining_position[None, :] >= 1, selected_entries, jnp.float32(0.0)) / SPAN_LENGTH
    local = jnp.cumsum(retained_rows.reshape(feature_width, N_ROWS, ROWS_DEV), axis=2)
    ends = local[:, :, -1]
    starts = jnp.cumsum(ends, axis=1) - ends
    running = (local + starts[:, :, None]).reshape(feature_width, total_rows)
    visited_tally = jnp.maximum(remaining_position.astype(jnp.float32), 1.0)
    deviation = lagging_mean - running / visited_tally[None, :]
    return lagging_mean, deviation


def reference(events, keep_indicator):
    lagging_mean, deviation = lax.map(single_table_input, (events, keep_indicator))
    return (lagging_mean, deviation)
```

```python
import jax
import jax.numpy as jnp
from jax import lax
from jax.experimental import pallas as pl
from jax.experimental.pallas import tpu as pltpu
from jax.sharding import Mesh
from jax.sharding import PartitionSpec as P

SPAN = 4096
LANES = 128
GROUP = 8
ROWS = ("rows_0", "rows_1", "rows_2", "rows_3")
SHAPE = (4, 4, 4, 2)
F32 = jnp.float32
I32 = jnp.int32
BF16 = jnp.bfloat16


def lanes_of(rows):
    return lax.broadcasted_iota(I32, (rows, LANES), 1)


def picked_lanes(values, index):
    return jnp.take_along_axis(values, index, axis=1, mode="promise_in_bounds")


def running_weights():
    row = lax.broadcasted_iota(I32, (2 * LANES, 2 * LANES), 0) & (LANES - 1)
    column = lax.broadcasted_iota(I32, (2 * LANES, 2 * LANES), 1)
    return ((row <= column) | (column >= LANES)).astype(F32).astype(BF16)


def index_tables(keep, flat, scalars, streams, tiles):
    count = streams * tiles
    for t in range(tiles):
        flat[t * streams : (t + 1) * streams, :] = keep[:, t * LANES : (t + 1) * LANES].astype(F32)
    flags = flat[...].astype(BF16)
    weights = running_weights()[:LANES]
    sums = jnp.dot(flags, weights, preferred_element_type=F32)
    within, total = (sums[:, :LANES], sums[:, LANES:])
    row = lax.broadcasted_iota(I32, (count, count), 0)
    column = lax.broadcasted_iota(I32, (count, count), 1)
    same = ((row ^ column) & (streams - 1)) == 0
    earlier = (same & (column < row)).astype(F32).astype(BF16)
    later = (same & (column > row)).astype(F32).astype(BF16)
    start = jnp.dot(earlier, total.astype(BF16), preferred_element_type=F32)
    line = lax.dot_general(
        jnp.ones((8, LANES), BF16), flags, (((1,), (1,)), ((), ())), preferred_element_type=F32
    )
    line_start = jnp.dot(line.astype(BF16), later, preferred_element_type=F32)
    sublane = lax.broadcasted_iota(I32, (8, count), 0)
    base = line_start + jnp.where(line == float(LANES), 1.0, 0.0)
    table = jnp.where(sublane == 0, line_start, jnp.where(sublane == 1, base, line_start + line))
    scalars[...] = table.astype(I32)
    begin = start.astype(I32)
    ordinal = ((lanes_of(count) - begin - 1) & (LANES - 1)).astype(F32)
    place = jnp.zeros((count, LANES), I32)
    step = LANES // 2
    while step:
        seen = picked_lanes(within, place + (step - 1))
        place = place + jnp.where(seen <= ordinal, step, 0)
        step //= 2
    return place, begin + within.astype(I32)


def pack_stream(s, streams, tiles, flat, events, index, starts, weights, work, prefix, local, tail):
    features = events.shape[0]
    lane = lanes_of(features)
    work[:, 0:LANES] = jnp.zeros((features, LANES), F32)

    def step(g, carry):
        tiles_in = []
        for j in range(GROUP):
            at = pl.multiple_of((g * GROUP + j) * LANES, LANES)
            kept = flat[pl.ds((g * GROUP + j) * streams + s, 1), :]
            tiles_in.append(events[:, pl.ds(at, LANES)] * kept)
        values = jnp.concatenate(tiles_in, axis=0)
        high = values.astype(BF16)
        low = (values - high.astype(F32)).astype(BF16)
        sums = jnp.dot(
            jnp.concatenate([high, low], axis=1), weights[...], preferred_element_type=F32
        )
        for j in range(GROUP):
            t = g * GROUP + j
            at = pl.multiple_of(t * LANES, LANES)
            block = sums[j * features : (j + 1) * features]
            running = carry + block[:, :LANES]
            carry = carry + block[:, LANES:]
            prefix[:, pl.ds(at, LANES)] = running
            order = jnp.broadcast_to(index[pl.ds(t * streams + s, 1), :], (features, LANES))
            packed = picked_lanes(running, order)
            slot = starts[0, t * streams + s] + 1
            low_at = pl.multiple_of((slot >> 7) * LANES, LANES)
            pltpu.store(
                work.at[:, pl.ds(low_at, LANES)], packed, mask=lane >= (slot & (LANES - 1))
            )
            work[:, pl.ds(low_at + LANES, LANES)] = packed
        return carry

    total = lax.fori_loop(0, tiles // GROUP, step, jnp.zeros((features, LANES), F32))
    local[...] = work[:, : SPAN + LANES]
    first = starts[2, (tiles - 1) * streams + s] - SPAN
    tile, shift = (first >> 7, first & (LANES - 1))
    turn = (LANES - shift) & (LANES - 1)
    from_first = lane < LANES - shift

    def turned(m):
        at = pl.multiple_of((tile + m) * LANES, LANES)
        return pltpu.roll(work[:, pl.ds(at, LANES)], turn, 1)

    before = turned(0)
    for m in range(SPAN // LANES):
        after = turned(m + 1)
        tail[:, m * LANES : (m + 1) * LANES] = jnp.where(from_first, before, after) - total
        before = after
    return total


def totals_line(s, total):
    features = total.shape[0]
    row = lax.broadcasted_iota(I32, (features, LANES), 0)
    chosen = jnp.where(lanes_of(features) == row + s * features, total, 0.0)
    return jnp.sum(chosen, axis=0, keepdims=True)


def pack_first_body(
    keep, events, flat, index, ranks, scalars, prefix, local, tail, totals,
    line, starts, weights, work, copied,
):
    streams, length = keep.shape
    tiles = length // LANES
    index[...], ranks[...] = index_tables(keep, flat, line, streams, tiles)
    copy = pltpu.make_async_copy(line, starts, copied)
    copy.start()
    weights[...] = running_weights()
    scalars[...] = line[...]
    copy.wait()
    total = pack_stream(
        0, streams, tiles, flat, events.at[0], index, starts, weights, work,
        prefix.at[0], local.at[0], tail.at[0],
    )
    sublane = lax.broadcasted_iota(I32, (8, LANES), 0)
    lane = lanes_of(8)
    counts = jnp.zeros((8, LANES), F32)
    for s in range(streams):
        counts = jnp.where(
            lane == s, starts[2, (tiles - 1) * streams + s].astype(F32), counts
        )
    line_of = jnp.broadcast_to(totals_line(0, total), (8, LANES))
    totals[...] = jnp.where(sublane == 0, line_of, jnp.where(sublane == 1, counts, 0.0))


def pack_rest_body(
    starts, flat, events, index, so_far, prefix, local, tail, totals, weights, work,
):
    tiles = events.shape[2] // LANES
    streams = flat.shape[0] // tiles
    step = pl.program_id(0)
    s = step + 1

    @pl.when(step == 0)
    def _():
        weights[...] = running_weights()
        totals[...] = so_far[...]

    total = pack_stream(
        s, streams, tiles, flat, events.at[0], index, starts, weights, work,
        prefix.at[0], local.at[0], tail.at[0],
    )
    sublane = lax.broadcasted_iota(I32, (8, LANES), 0)
    line_of = jnp.broadcast_to(totals_line(s, total), (8, LANES))
    totals[...] = totals[...] + jnp.where(sublane == 0, line_of, 0.0)


def carried_body(before, ranks, columns, scale):
    streams, features, _ = columns.shape
    sums = before[0:1, :]
    row = lax.broadcasted_iota(I32, (features, LANES), 0)
    for s in range(streams):
        chosen = jnp.where(lanes_of(features) == row + s * features, sums, 0.0)
        columns[s] = jnp.broadcast_to(jnp.sum(chosen, axis=1, keepdims=True), (features, LANES))
    count = ranks.shape[0]
    stream = lax.broadcasted_iota(I32, (count, LANES), 0) & (streams - 1)
    seen = jnp.zeros((count, LANES), F32)
    for s in range(streams):
        tally = jnp.sum(jnp.where(lanes_of(1) == s, before[1:2, :], 0.0))
        seen = jnp.where(stream == s, tally, seen)
    scale[...] = 1.0 / jnp.maximum(seen + ranks[...].astype(F32), 1.0)


def spread_body(first, streams, starts, arrived, local, prefix, ranks, scale, columns, *refs):
    lagging, deviation, joint = refs[-3:]
    features, length = prefix.shape[1:]
    tiles = length // LANES
    s = first + pl.program_id(0)
    block = pl.program_id(1)
    lane = lanes_of(features)

    @pl.when(block == 0)
    def _():
        joint[:, :SPAN] = arrived[0]
        joint[:, SPAN:] = local[0]

    before = columns[s]

    def step(g, carry):
        for j in range(GROUP):
            t = g * GROUP + j
            row = (block * tiles + t) * streams + s
            at = pl.multiple_of(t * LANES, LANES)
            base = starts[1, row]
            low_at = pl.multiple_of((base >> 7) * LANES, LANES)
            window = jnp.where(
                lane >= (base & (LANES - 1)),
                joint[:, pl.ds(low_at, LANES)],
                joint[:, pl.ds(low_at + LANES, LANES)],
            )
            order = jnp.broadcast_to(ranks[pl.ds(row, 1), :] & (LANES - 1), (features, LANES))
            running = prefix[0, :, pl.ds(at, LANES)]
            mean = (running - picked_lanes(window, order)) * (1.0 / SPAN)
            lagging[0, :, pl.ds(at, LANES)] = mean
            deviation[0, :, pl.ds(at, LANES)] = mean - (before + running) * scale[pl.ds(row, 1), :]
        return carry

    lax.fori_loop(0, tiles // GROUP, step, 0)


def whole(shape):
    return pl.BlockSpec(shape, lambda *_: (0,) * len(shape))


SMEM_WHOLE = pl.BlockSpec(memory_space=pltpu.SMEM)


def pack_first(keep, events):
    streams, features, length = events.shape
    count = streams * length // LANES
    shapes = [
        jax.ShapeDtypeStruct((count, LANES), F32),
        jax.ShapeDtypeStruct((count, LANES), I32),
        jax.ShapeDtypeStruct((count, LANES), I32),
        jax.ShapeDtypeStruct((8, count), I32),
        jax.ShapeDtypeStruct((1, features, length), F32),
        jax.ShapeDtypeStruct((1, features, SPAN + LANES), F32),
        jax.ShapeDtypeStruct((1, features, SPAN), F32),
        jax.ShapeDtypeStruct((8, LANES), F32),
    ]
    return pl.pallas_call(
        pack_first_body,
        grid=(1,),
        in_specs=[whole((streams, length)), whole((1, features, length))],
        out_specs=[whole(shape.shape) for shape in shapes],
        out_shape=shapes,
        scratch_shapes=[
            pltpu.VMEM((8, count), I32),
            pltpu.SMEM((8, count), I32),
            pltpu.VMEM((2 * LANES, 2 * LANES), BF16),
            pltpu.VMEM((features, length + LANES), F32),
            pltpu.SemaphoreType.DMA,
        ],
        name="pack_first",
    )(keep, events)


def pack_rest(starts, flat, events, index, so_far):
    streams, features, length = events.shape
    rest = streams - 1

    def one(width):
        return pl.BlockSpec((1, features, width), lambda i: (i, 0, 0))

    return pl.pallas_call(
        pack_rest_body,
        grid=(rest,),
        in_specs=[
            SMEM_WHOLE,
            whole(flat.shape),
            pl.BlockSpec((1, features, length), lambda i: (i + 1, 0, 0)),
            whole(index.shape),
            whole((8, LANES)),
        ],
        out_specs=[one(length), one(SPAN + LANES), one(SPAN), whole((8, LANES))],
        out_shape=[
            jax.ShapeDtypeStruct((rest, features, length), F32),
            jax.ShapeDtypeStruct((rest, features, SPAN + LANES), F32),
            jax.ShapeDtypeStruct((rest, features, SPAN), F32),
            jax.ShapeDtypeStruct((8, LANES), F32),
        ],
        scratch_shapes=[
            pltpu.VMEM((2 * LANES, 2 * LANES), BF16),
            pltpu.VMEM((features, length + LANES), F32),
        ],
        name="pack_rest",
    )(starts, flat, events, index, so_far)


def carried(before, ranks, streams, features):
    return pl.pallas_call(
        carried_body,
        out_shape=[
            jax.ShapeDtypeStruct((streams, features, LANES), F32),
            jax.ShapeDtypeStruct(ranks.shape, F32),
        ],
        name="carried",
    )(before, ranks)


def spread(first, streams, starts, arrived, local, prefix, ranks, scale, columns, outputs):
    number, features, length = prefix.shape
    halves = 2
    block = pl.BlockSpec((1, features, length // halves), lambda i, h: (i, 0, h))
    placed = pl.BlockSpec((1, features, length // halves), lambda i, h: (first + i, 0, h))

    def one(width):
        return pl.BlockSpec((1, features, width), lambda i, h: (i, 0, 0))

    def body(*refs):
        spread_body(first, streams, *refs)

    given = [] if outputs is None else list(outputs)
    return pl.pallas_call(
        body,
        grid=(number, halves),
        in_specs=[
            SMEM_WHOLE,
            one(SPAN),
            one(SPAN + LANES),
            block,
            whole(ranks.shape),
            whole(scale.shape),
            whole(columns.shape),
            *[pl.BlockSpec(memory_space=pl.ANY) for _ in given],
        ],
        out_specs=[placed, placed],
        out_shape=[jax.ShapeDtypeStruct((streams, features, length), F32)] * 2,
        scratch_shapes=[pltpu.VMEM((features, 2 * SPAN + LANES), F32)],
        input_output_aliases={7 + k: k for k in range(len(given))},
        name="spread",
    )(starts, arrived, local, prefix, ranks, scale, columns, *given)


def exchanged(totals):
    before = jnp.zeros_like(totals)
    for axis in reversed(ROWS):
        count, position = (lax.axis_size(axis), lax.axis_index(axis))
        bit = 1
        while bit < count:
            other = lax.ppermute(totals, axis, [(k, k ^ bit) for k in range(count)])
            before = before + jnp.where(position & bit, other, 0.0)
            totals = totals + other
            bit *= 2
    return before


def from_behind(value):
    count = lax.axis_size(ROWS)
    return lax.ppermute(value, ROWS, [(k, k + 1) for k in range(count - 1)])


def per_device(events, keep):
    streams, features, _ = events.shape
    flat, index, ranks, starts, prefix_a, local_a, tail_a, totals = pack_first(keep, events)
    arrived_a = from_behind(tail_a)
    prefix_b, local_b, tail_b, totals = pack_rest(starts, flat, events, index, totals)
    arrived_b = from_behind(tail_b)
    columns, scale = carried(exchanged(totals), ranks, streams, features)
    outputs = spread(
        0, streams, starts, arrived_a, local_a, prefix_a, ranks, scale, columns, None
    )
    return tuple(
        spread(1, streams, starts, arrived_b, local_b, prefix_b, ranks, scale, columns, outputs)
    )


def solution(mesh):
    shape = SHAPE if mesh.size == 128 else (1, 1, mesh.size // 2, 2)
    finer = Mesh(mesh.devices.reshape(shape), ROWS)
    in_specs = (P(None, None, ROWS), P(None, ROWS))
    out_specs = (P(None, None, ROWS), P(None, None, ROWS))
    return jax.shard_map(
        per_device, mesh=finer, in_specs=in_specs, out_specs=out_specs, check_vma=False
    )
```

```python
import jax
import jax.numpy as jnp
from jax import lax
from jax.experimental import pallas as pl
from jax.experimental.pallas import tpu as pltpu
from jax.sharding import Mesh
from jax.sharding import PartitionSpec as P


SPAN = 4096
LANES = 128
GROUP = 32
GROUP_SUM = 8
ROWS = ("rows_0", "rows_1", "rows_2", "rows_3")
SHAPE = (4, 4, 4, 2)
F32 = jnp.float32
I32 = jnp.int32
BF16 = jnp.bfloat16


def lanes_of(rows):
    return lax.broadcasted_iota(I32, (rows, LANES), 1)


def picked_lanes(values, index):
    return jnp.take_along_axis(values, index, axis=1, mode="promise_in_bounds")


def running_weights():
    row = lax.broadcasted_iota(I32, (2 * LANES, 2 * LANES), 0) & (LANES - 1)
    column = lax.broadcasted_iota(I32, (2 * LANES, 2 * LANES), 1)
    return ((row <= column) | (column >= LANES)).astype(F32).astype(BF16)


def index_tables(keep, flat, scalars, streams, tiles):
    count = streams * tiles
    for t in range(tiles):
        flat[t * streams : (t + 1) * streams, :] = keep[:, t * LANES : (t + 1) * LANES].astype(F32)
    flags = flat[...].astype(BF16)
    weights = running_weights()[:LANES]
    sums = jnp.dot(flags, weights, preferred_element_type=F32)
    within, total = (sums[:, :LANES], sums[:, LANES:])
    row = lax.broadcasted_iota(I32, (count, count), 0)
    column = lax.broadcasted_iota(I32, (count, count), 1)
    same = ((row ^ column) & (streams - 1)) == 0
    earlier = (same & (column < row)).astype(F32).astype(BF16)
    later = (same & (column > row)).astype(F32).astype(BF16)
    start = jnp.dot(earlier, total.astype(BF16), preferred_element_type=F32)
    line = lax.dot_general(
        jnp.ones((8, LANES), BF16), flags, (((1,), (1,)), ((), ())), preferred_element_type=F32
    )
    line_start = jnp.dot(line.astype(BF16), later, preferred_element_type=F32)
    sublane = lax.broadcasted_iota(I32, (8, count), 0)
    base = line_start + jnp.where(line == float(LANES), 1.0, 0.0)
    table = jnp.where(sublane == 0, line_start, jnp.where(sublane == 1, base, line_start + line))
    scalars[...] = table.astype(I32)
    begin = start.astype(I32)
    ordinal = ((lanes_of(count) - begin - 1) & (LANES - 1)).astype(F32)
    place = jnp.zeros((count, LANES), I32)
    step = LANES // 2
    while step:
        seen = picked_lanes(within, place + (step - 1))
        place = place + jnp.where(seen <= ordinal, step, 0)
        step //= 2
    return place, begin + within.astype(I32)


def pack_stream(s, streams, tiles, flat, state, index, starts, work, tail):
    features = state.shape[0]
    lane = lanes_of(features)
    weights = running_weights()
    work[:, 0:LANES] = jnp.zeros((features, LANES), F32)

    def step(g, carry):
        tiles_in = []
        for j in range(GROUP):
            at = pl.multiple_of((g * GROUP + j) * LANES, LANES)
            kept = flat[pl.ds((g * GROUP + j) * streams + s, 1), :]
            tiles_in.append(state[:, pl.ds(at, LANES)] * kept)
        values = jnp.concatenate(tiles_in, axis=0)
        high = values.astype(BF16)
        low = (values - high.astype(F32)).astype(BF16)
        sums = jnp.dot(
            jnp.concatenate([high, low], axis=1), weights, preferred_element_type=F32
        )
        for j in range(GROUP):
            t = g * GROUP + j
            at = pl.multiple_of(t * LANES, LANES)
            block = sums[j * features : (j + 1) * features]
            running = carry + block[:, :LANES]
            carry = carry + block[:, LANES:]
            state[:, pl.ds(at, LANES)] = running
            order = jnp.broadcast_to(index[pl.ds(t * streams + s, 1), :], (features, LANES))
            packed = picked_lanes(running, order)
            slot = starts[0, t * streams + s] + 1
            low_at = pl.multiple_of((slot >> 7) * LANES, LANES)
            pltpu.store(
                work.at[:, pl.ds(low_at, LANES)], packed, mask=lane >= (slot & (LANES - 1))
            )
            work[:, pl.ds(low_at + LANES, LANES)] = packed
        return carry

    total = lax.fori_loop(0, tiles // GROUP, step, jnp.zeros((features, LANES), F32))
    state[:, tiles * LANES : tiles * LANES + SPAN + LANES] = work[:, : SPAN + LANES]
    first = starts[2, (tiles - 1) * streams + s] - SPAN
    tile, shift = (first >> 7, first & (LANES - 1))
    turn = (LANES - shift) & (LANES - 1)
    from_first = lane < LANES - shift

    def turned(m):
        at = pl.multiple_of((tile + m) * LANES, LANES)
        return pltpu.roll(work[:, pl.ds(at, LANES)], turn, 1)

    before = turned(0)
    for m in range(SPAN // LANES):
        after = turned(m + 1)
        tail[:, m * LANES : (m + 1) * LANES] = jnp.where(from_first, before, after) - total
        before = after
    return total


def totals_line(s, total):
    features = total.shape[0]
    row = lax.broadcasted_iota(I32, (features, LANES), 0)
    chosen = jnp.where(lanes_of(features) == row + s * features, total, 0.0)
    return jnp.sum(chosen, axis=0, keepdims=True)


def pack_first_body(
    keep_hbm, events, state, flat, index, ranks, scalars, tail, totals,
    keep, starts, work, copied, loaded,
):
    streams, length = keep.shape
    features = events.shape[1]
    tiles = length // LANES
    loads = [
        pltpu.make_async_copy(events.at[s], state.at[s, :, pl.ds(0, length)], loaded.at[s])
        for s in range(streams)
    ]
    flags = pltpu.make_async_copy(keep_hbm, keep, copied)
    flags.start()
    for load in loads:
        load.start()
    flags.wait()
    index[...], ranks[...] = index_tables(keep, flat, scalars, streams, tiles)
    copy = pltpu.make_async_copy(scalars, starts, copied)
    copy.start()
    copy.wait()
    loads[0].wait()
    total = pack_stream(
        0, streams, tiles, flat, state.at[0], index, starts, work, tail.at[0]
    )
    for load in loads[1:]:
        load.wait()

    def step(g, sums):
        sums = list(sums)
        for j in range(GROUP_SUM):
            t = g * GROUP_SUM + j
            at = pl.multiple_of(t * LANES, LANES)
            for s in range(1, streams):
                kept = state[s, :, pl.ds(at, LANES)] * flat[pl.ds(t * streams + s, 1), :]
                sums[s - 1] = sums[s - 1] + kept
        return tuple(sums)

    zero = jnp.zeros((features, LANES), F32)
    sums = lax.fori_loop(0, tiles // GROUP_SUM, step, (zero,) * (streams - 1))
    sublane = lax.broadcasted_iota(I32, (8, LANES), 0)
    lane = lanes_of(8)
    counts = jnp.zeros((8, LANES), F32)
    for s in range(streams):
        counts = jnp.where(lane == s, starts[2, (tiles - 1) * streams + s].astype(F32), counts)
    line = totals_line(0, total)
    for s in range(1, streams):
        whole_sum = jnp.broadcast_to(
            jnp.sum(sums[s - 1], axis=1, keepdims=True), (features, LANES)
        )
        line = line + totals_line(s, whole_sum)
    line = jnp.broadcast_to(line, (8, LANES))
    totals[...] = jnp.where(sublane == 0, line, jnp.where(sublane == 1, counts, 0.0))


def spread_stream(s, at_stream, streams, length, starts, arrived, state, ranks, joint):
    features = state.shape[1]
    lane = lanes_of(features)
    joint[:, :SPAN] = jnp.where(lax.axis_index(ROWS) > 0, arrived[at_stream], 0.0)
    joint[:, SPAN:] = state[s, :, length : length + SPAN + LANES]

    def step(g, carry):
        for j in range(GROUP):
            t = g * GROUP + j
            row = t * streams + s
            at = pl.multiple_of(t * LANES, LANES)
            base = starts[1, row]
            low_at = pl.multiple_of((base >> 7) * LANES, LANES)
            window = jnp.where(
                lane >= (base & (LANES - 1)),
                joint[:, pl.ds(low_at, LANES)],
                joint[:, pl.ds(low_at + LANES, LANES)],
            )
            order = jnp.broadcast_to(ranks[pl.ds(row, 1), :] & (LANES - 1), (features, LANES))
            running = state[s, :, pl.ds(at, LANES)]
            state[s, :, pl.ds(length + at, LANES)] = (
                running - picked_lanes(window, order)
            ) * (1.0 / SPAN)
        return carry

    lax.fori_loop(0, length // LANES // GROUP, step, 0)


def means_of(s, length, state):
    return state.at[s, :, pl.ds(length, length)]


def gathered(totals_of):
    before = jnp.zeros(totals_of[0].shape, F32)
    number = 0
    for axis in reversed(ROWS):
        count, position = (lax.axis_size(axis), lax.axis_index(axis))
        if axis == ROWS[2]:
            for step in range(1, count):
                taken = (position + step >= count).astype(F32)
                before = before + totals_of[number][...] * taken
                number += 1
            continue
        bit = 1
        while bit < count:
            taken = ((position & bit) != 0).astype(F32)
            before = before + totals_of[number][...] * taken
            number += 1
            bit *= 2
    return before


IN_VMEM = pl.BlockSpec(memory_space=pltpu.VMEM)
IN_SMEM = pl.BlockSpec(memory_space=pltpu.SMEM)
IN_HBM = pl.BlockSpec(memory_space=pltpu.HBM)
PARAMS = pltpu.CompilerParams(vmem_limit_bytes=12 << 20)


def pack_first(keep, events):
    streams, features, length = events.shape
    count = streams * length // LANES
    shapes = [
        pltpu.VMEM((streams, features, 2 * length), F32),
        pltpu.VMEM((count, LANES), F32),
        pltpu.VMEM((count, LANES), I32),
        pltpu.VMEM((count, LANES), I32),
        pltpu.VMEM((8, count), I32),
        pltpu.VMEM((1, features, SPAN), F32),
        pltpu.VMEM((8, LANES), F32),
    ]
    return pl.pallas_call(
        pack_first_body,
        in_specs=[IN_HBM, IN_HBM],
        out_specs=[IN_VMEM] * len(shapes),
        out_shape=shapes,
        scratch_shapes=[
            pltpu.VMEM((streams, length), I32),
            pltpu.SMEM((8, count), I32),
            pltpu.VMEM((features, length + LANES), F32),
            pltpu.SemaphoreType.DMA,
            pltpu.SemaphoreType.DMA((streams,)),
        ],
        compiler_params=PARAMS,
        name="pack_first",
    )(
        pltpu.with_memory_space_constraint(keep, pltpu.HBM),
        pltpu.with_memory_space_constraint(events, pltpu.HBM),
    )


def pack(s, length, starts, flat, state, index, slot, number, shared=None):
    streams, features, _ = state.shape
    tiles = length // LANES

    def body(starts, flat, _, index, *refs):
        state, tail, work = refs[-3:]
        pack_stream(s, streams, tiles, flat, state.at[s], index, starts, work, tail.at[slot])

    given = [] if shared is None else [shared]
    return pl.pallas_call(
        body,
        in_specs=[IN_SMEM] + [IN_VMEM] * (3 + len(given)),
        out_specs=[IN_VMEM] * 2,
        out_shape=[
            pltpu.VMEM(state.shape, F32),
            pltpu.VMEM((number, features, SPAN), F32),
        ],
        scratch_shapes=[pltpu.VMEM((features, length + LANES), F32)],
        input_output_aliases={2: 0, **{4 + k: 1 for k in range(len(given))}},
        compiler_params=PARAMS,
        name="pack",
    )(starts, flat, state, index, *given)


def spread(s, at_stream, length, starts, arrived, state, ranks, lagging):
    streams, features, _ = state.shape

    def body(starts, arrived, _, ranks, *refs):
        *outs, joint, sent = refs[-4:] if s else (None,) + refs[-3:]
        state = outs[-2] if s else outs[-1]
        write = None
        if s:
            write = pltpu.make_async_copy(means_of(s - 1, length, state), outs[-1].at[s - 1], sent)
            write.start()
        spread_stream(s, at_stream, streams, length, starts, arrived, state, ranks, joint)
        if write is not None:
            write.wait()

    given = [] if lagging is None else [lagging]
    out_shape = [pltpu.VMEM(state.shape, F32)]
    if s:
        out_shape.append(jax.ShapeDtypeStruct((streams, features, length), F32))
    results = pl.pallas_call(
        body,
        in_specs=[IN_SMEM] + [IN_VMEM] * 3 + [IN_HBM] * len(given),
        out_specs=[IN_VMEM, IN_HBM][: len(out_shape)],
        out_shape=out_shape,
        scratch_shapes=[
            pltpu.VMEM((features, 2 * SPAN + LANES), F32),
            pltpu.SemaphoreType.DMA,
        ],
        input_output_aliases={2: 0, **{4 + k: 1 for k in range(len(given))}},
        compiler_params=PARAMS,
        name="spread",
    )(starts, arrived, state, ranks, *given)
    return (results[0], results[1] if s else None)


def finish(at_stream, length, starts, arrived, state, ranks, lagging, totals_of):
    streams, features, _ = state.shape
    last = streams - 1
    tiles = length // LANES
    count = ranks.shape[0]

    def body(starts, arrived, _, ranks, __, *refs):
        totals_of = refs[: len(refs) - 9]
        state, lagging, deviation, joint, columns, scale, staged, sent, gone = refs[-9:]
        writes = [
            pltpu.make_async_copy(
                means_of(last - 1, length, state), lagging.at[last - 1], sent.at[0]
            )
        ]
        writes[0].start()
        before = gathered(totals_of)
        sums = before[0:1, :]
        row = lax.broadcasted_iota(I32, (features, LANES), 0)
        for s in range(streams):
            chosen = jnp.where(lanes_of(features) == row + s * features, sums, 0.0)
            columns[s] = jnp.broadcast_to(
                jnp.sum(chosen, axis=1, keepdims=True), (features, LANES)
            )
        stream = lax.broadcasted_iota(I32, (count, LANES), 0) & (streams - 1)
        seen = jnp.zeros((count, LANES), F32)
        for s in range(streams):
            tally = jnp.sum(jnp.where(lanes_of(1) == s, before[1:2, :], 0.0))
            seen = jnp.where(stream == s, tally, seen)
        scale[...] = 1.0 / jnp.maximum(seen + ranks[...].astype(F32), 1.0)

        def deviate(s):
            column = columns[s]

            def step(g, carry):
                for j in range(GROUP):
                    t = g * GROUP + j
                    at = pl.multiple_of(t * LANES, LANES)
                    running = state[s, :, pl.ds(at, LANES)]
                    staged[s, :, pl.ds(at, LANES)] = state[s, :, pl.ds(length + at, LANES)] - (
                        column + running
                    ) * scale[pl.ds(t * streams + s, 1), :]
                return carry

            lax.fori_loop(0, tiles // GROUP, step, 0)
            write = pltpu.make_async_copy(staged.at[s], deviation.at[s], gone.at[s])
            write.start()
            writes.append(write)

        for s in range(last):
            deviate(s)
        spread_stream(last, at_stream, streams, length, starts, arrived, state, ranks, joint)
        write = pltpu.make_async_copy(means_of(last, length, state), lagging.at[last], sent.at[1])
        write.start()
        writes.append(write)
        deviate(last)
        for write in writes:
            write.wait()

    shape = jax.ShapeDtypeStruct((streams, features, length), F32)
    _, lagging, deviation = pl.pallas_call(
        body,
        in_specs=[IN_SMEM] + [IN_VMEM] * 3 + [IN_HBM] + [IN_VMEM] * len(totals_of),
        out_specs=[IN_VMEM, IN_HBM, IN_HBM],
        out_shape=[pltpu.VMEM(state.shape, F32), shape, shape],
        scratch_shapes=[
            pltpu.VMEM((features, 2 * SPAN + LANES), F32),
            pltpu.VMEM((streams, features, LANES), F32),
            pltpu.VMEM((count, LANES), F32),
            pltpu.VMEM((streams, features, length), F32),
            pltpu.SemaphoreType.DMA((2,)),
            pltpu.SemaphoreType.DMA((streams,)),
        ],
        input_output_aliases={2: 0, 4: 1},
        compiler_params=PARAMS,
        name="finish",
    )(starts, arrived, state, ranks, lagging, *totals_of)
    return (lagging, deviation)


def exchanged(totals):
    brought = []
    for axis in reversed(ROWS):
        count = lax.axis_size(axis)
        moving = totals
        bit = 1
        for _ in range(1, count):
            if axis == ROWS[2]:
                pairs = [(k, (k - 1) % count) for k in range(count)]
            elif bit < count:
                pairs = [(k, k ^ (2 * bit - 1)) for k in range(count)]
                moving = totals
                bit *= 2
            else:
                break
            moving = lax.ppermute(moving, axis, pairs)
            brought.append(moving)
            totals = totals + moving
    return brought


def from_behind(value):
    count = lax.axis_size(ROWS)
    return lax.ppermute(value, ROWS, [(k, (k + 1) % count) for k in range(count)])


def per_device(events, keep):
    streams, _, length = events.shape
    state, flat, index, ranks, starts, tail, totals = pack_first(keep, events)
    arrived = {0: (from_behind(tail), 0)}
    state, tail = pack(1, length, starts, flat, state, index, 0, 2)
    state, tail = pack(2, length, starts, flat, state, index, 1, 2, tail)
    there = from_behind(tail)
    arrived.update({1: (there, 0), 2: (there, 1)})
    state, tail = pack(3, length, starts, flat, state, index, 0, 1)
    arrived[3] = (from_behind(tail), 0)
    totals_of = exchanged(totals)
    lagging = None
    for s in range(streams - 1):
        there, k = arrived[s]
        state, lagging = spread(s, k, length, starts, there, state, ranks, lagging)
    there, k = arrived[streams - 1]
    return finish(k, length, starts, there, state, ranks, lagging, totals_of)


def solution(mesh):
    shape = SHAPE if mesh.size == 128 else (1, 1, mesh.size // 2, 2)
    finer = Mesh(mesh.devices.reshape(shape), ROWS)
    in_specs = (P(None, None, ROWS), P(None, ROWS))
    out_specs = (P(None, None, ROWS), P(None, None, ROWS))
    return jax.shard_map(
        per_device, mesh=finer, in_specs=in_specs, out_specs=out_specs, check_vma=False
    )
```

```python
import jax
import jax.numpy as jnp
from jax import lax
from jax.experimental import pallas as pl
from jax.experimental.pallas import tpu as pltpu
from jax.sharding import Mesh
from jax.sharding import PartitionSpec as P


SPAN = 4096
LANES = 128
GROUP = 32
GROUP_SUM = 8
ROWS = ("rows_0", "rows_1", "rows_2", "rows_3")
SHAPE = (4, 4, 4, 2)
F32 = jnp.float32
I32 = jnp.int32
BF16 = jnp.bfloat16


def lanes_of(rows):
    return lax.broadcasted_iota(I32, (rows, LANES), 1)


def picked_lanes(values, index):
    return jnp.take_along_axis(values, index, axis=1, mode="promise_in_bounds")


def running_weights():
    row = lax.broadcasted_iota(I32, (2 * LANES, 2 * LANES), 0) & (LANES - 1)
    column = lax.broadcasted_iota(I32, (2 * LANES, 2 * LANES), 1)
    return ((row <= column) | (column >= LANES)).astype(F32).astype(BF16)


def index_tables(keep, flat, scalars, streams, tiles):
    count = streams * tiles
    for t in range(tiles):
        flat[t * streams : (t + 1) * streams, :] = keep[:, t * LANES : (t + 1) * LANES].astype(F32)
    flags = flat[...].astype(BF16)
    weights = running_weights()[:LANES]
    sums = jnp.dot(flags, weights, preferred_element_type=F32)
    within, total = (sums[:, :LANES], sums[:, LANES:])
    row = lax.broadcasted_iota(I32, (count, count), 0)
    column = lax.broadcasted_iota(I32, (count, count), 1)
    same = ((row ^ column) & (streams - 1)) == 0
    earlier = (same & (column < row)).astype(F32).astype(BF16)
    later = (same & (column > row)).astype(F32).astype(BF16)
    start = jnp.dot(earlier, total.astype(BF16), preferred_element_type=F32)
    line = lax.dot_general(
        jnp.ones((8, LANES), BF16), flags, (((1,), (1,)), ((), ())), preferred_element_type=F32
    )
    line_start = jnp.dot(line.astype(BF16), later, preferred_element_type=F32)
    sublane = lax.broadcasted_iota(I32, (8, count), 0)
    base = line_start + jnp.where(line == float(LANES), 1.0, 0.0)
    table = jnp.where(sublane == 0, line_start, jnp.where(sublane == 1, base, line_start + line))
    scalars[...] = table.astype(I32)
    begin = start.astype(I32)
    ordinal = ((lanes_of(count) - begin - 1) & (LANES - 1)).astype(F32)
    place = jnp.zeros((count, LANES), I32)
    step = LANES // 2
    while step:
        seen = picked_lanes(within, place + (step - 1))
        place = place + jnp.where(seen <= ordinal, step, 0)
        step //= 2
    return place, begin + within.astype(I32)


def pack_stream(s, streams, tiles, flat, state, index, starts, work, tail):
    features = state.shape[0]
    lane = lanes_of(features)
    weights = running_weights()
    work[:, 0:LANES] = jnp.zeros((features, LANES), F32)

    def step(g, carry):
        tiles_in = []
        for j in range(GROUP):
            at = pl.multiple_of((g * GROUP + j) * LANES, LANES)
            kept = flat[pl.ds((g * GROUP + j) * streams + s, 1), :]
            tiles_in.append(state[:, pl.ds(at, LANES)] * kept)
        values = jnp.concatenate(tiles_in, axis=0)
        high = values.astype(BF16)
        low = (values - high.astype(F32)).astype(BF16)
        sums = jnp.dot(
            jnp.concatenate([high, low], axis=1), weights, preferred_element_type=F32
        )
        for j in range(GROUP):
            t = g * GROUP + j
            at = pl.multiple_of(t * LANES, LANES)
            block = sums[j * features : (j + 1) * features]
            running = carry + block[:, :LANES]
            carry = carry + block[:, LANES:]
            state[:, pl.ds(at, LANES)] = running
            order = jnp.broadcast_to(index[pl.ds(t * streams + s, 1), :], (features, LANES))
            packed = picked_lanes(running, order)
            slot = starts[0, t * streams + s] + 1
            low_at = pl.multiple_of((slot >> 7) * LANES, LANES)
            pltpu.store(
                work.at[:, pl.ds(low_at, LANES)], packed, mask=lane >= (slot & (LANES - 1))
            )
            work[:, pl.ds(low_at + LANES, LANES)] = packed
        return carry

    total = lax.fori_loop(0, tiles // GROUP, step, jnp.zeros((features, LANES), F32))
    state[:, tiles * LANES : tiles * LANES + SPAN + LANES] = work[:, : SPAN + LANES]
    first = starts[2, (tiles - 1) * streams + s] - SPAN
    tile, shift = (first >> 7, first & (LANES - 1))
    turn = (LANES - shift) & (LANES - 1)
    from_first = lane < LANES - shift

    def turned(m):
        at = pl.multiple_of((tile + m) * LANES, LANES)
        return pltpu.roll(work[:, pl.ds(at, LANES)], turn, 1)

    before = turned(0)
    for m in range(SPAN // LANES):
        after = turned(m + 1)
        tail[:, m * LANES : (m + 1) * LANES] = jnp.where(from_first, before, after) - total
        before = after
    return total


def totals_line(s, total):
    features = total.shape[0]
    row = lax.broadcasted_iota(I32, (features, LANES), 0)
    chosen = jnp.where(lanes_of(features) == row + s * features, total, 0.0)
    return jnp.sum(chosen, axis=0, keepdims=True)


def pack_first_body(
    keep_hbm, events, state, flat, index, ranks, scalars, tail, totals,
    keep, starts, work, copied, loaded,
):
    streams, length = keep.shape
    features = events.shape[1]
    tiles = length // LANES
    loads = [
        pltpu.make_async_copy(events.at[s], state.at[s, :, pl.ds(0, length)], loaded.at[s])
        for s in range(streams)
    ]
    flags = pltpu.make_async_copy(keep_hbm, keep, copied)
    flags.start()
    for load in loads:
        load.start()
    flags.wait()
    index[...], ranks[...] = index_tables(keep, flat, scalars, streams, tiles)
    copy = pltpu.make_async_copy(scalars, starts, copied)
    copy.start()
    copy.wait()
    loads[0].wait()
    total = pack_stream(
        0, streams, tiles, flat, state.at[0], index, starts, work, tail.at[0]
    )
    for load in loads[1:]:
        load.wait()

    def step(g, sums):
        sums = list(sums)
        for j in range(GROUP_SUM):
            t = g * GROUP_SUM + j
            at = pl.multiple_of(t * LANES, LANES)
            for s in range(1, streams):
                kept = state[s, :, pl.ds(at, LANES)] * flat[pl.ds(t * streams + s, 1), :]
                sums[s - 1] = sums[s - 1] + kept
        return tuple(sums)

    zero = jnp.zeros((features, LANES), F32)
    sums = lax.fori_loop(0, tiles // GROUP_SUM, step, (zero,) * (streams - 1))
    sublane = lax.broadcasted_iota(I32, (8, LANES), 0)
    lane = lanes_of(8)
    counts = jnp.zeros((8, LANES), F32)
    for s in range(streams):
        counts = jnp.where(lane == s, starts[2, (tiles - 1) * streams + s].astype(F32), counts)
    line = totals_line(0, total)
    for s in range(1, streams):
        whole_sum = jnp.broadcast_to(
            jnp.sum(sums[s - 1], axis=1, keepdims=True), (features, LANES)
        )
        line = line + totals_line(s, whole_sum)
    line = jnp.broadcast_to(line, (8, LANES))
    totals[...] = jnp.where(sublane == 0, line, jnp.where(sublane == 1, counts, 0.0))


def spread_stream(s, at_stream, streams, length, starts, arrived, state, ranks, joint):
    features = state.shape[1]
    lane = lanes_of(features)
    joint[:, :SPAN] = jnp.where(lax.axis_index(ROWS) > 0, arrived[at_stream], 0.0)
    joint[:, SPAN:] = state[s, :, length : length + SPAN + LANES]

    def step(g, carry):
        for j in range(GROUP):
            t = g * GROUP + j
            row = t * streams + s
            at = pl.multiple_of(t * LANES, LANES)
            base = starts[1, row]
            low_at = pl.multiple_of((base >> 7) * LANES, LANES)
            window = jnp.where(
                lane >= (base & (LANES - 1)),
                joint[:, pl.ds(low_at, LANES)],
                joint[:, pl.ds(low_at + LANES, LANES)],
            )
            order = jnp.broadcast_to(ranks[pl.ds(row, 1), :] & (LANES - 1), (features, LANES))
            running = state[s, :, pl.ds(at, LANES)]
            state[s, :, pl.ds(length + at, LANES)] = (
                running - picked_lanes(window, order)
            ) * (1.0 / SPAN)
        return carry

    lax.fori_loop(0, length // LANES // GROUP, step, 0)


def means_of(s, length, state):
    return state.at[s, :, pl.ds(length, length)]


def taken(axis, bit):
    return ((lax.axis_index(axis) & bit) != 0).astype(F32)


def earlier_rows(brought, axis):
    number = len(brought)
    return sum(
        (brought[k][0:2, :] * taken(axis, 1 << k) for k in range(number)), jnp.zeros((2, LANES), F32)
    )


IN_VMEM = pl.BlockSpec(memory_space=pltpu.VMEM)
IN_SMEM = pl.BlockSpec(memory_space=pltpu.SMEM)
IN_HBM = pl.BlockSpec(memory_space=pltpu.HBM)
PARAMS = pltpu.CompilerParams(vmem_limit_bytes=12 << 20)


def pack_first(keep, events):
    streams, features, length = events.shape
    count = streams * length // LANES
    shapes = [
        pltpu.VMEM((streams, features, 2 * length), F32),
        pltpu.VMEM((count, LANES), F32),
        pltpu.VMEM((count, LANES), I32),
        pltpu.VMEM((count, LANES), I32),
        pltpu.VMEM((8, count), I32),
        pltpu.VMEM((1, features, SPAN), F32),
        pltpu.VMEM((8, LANES), F32),
    ]
    return pl.pallas_call(
        pack_first_body,
        in_specs=[IN_HBM, IN_HBM],
        out_specs=[IN_VMEM] * len(shapes),
        out_shape=shapes,
        scratch_shapes=[
            pltpu.VMEM((streams, length), I32),
            pltpu.SMEM((8, count), I32),
            pltpu.VMEM((features, length + LANES), F32),
            pltpu.SemaphoreType.DMA,
            pltpu.SemaphoreType.DMA((streams,)),
        ],
        compiler_params=PARAMS,
        name="pack_first",
    )(
        pltpu.with_memory_space_constraint(keep, pltpu.HBM),
        pltpu.with_memory_space_constraint(events, pltpu.HBM),
    )


def pack(s, length, starts, flat, state, index, slot, number, shared=None):
    streams, features, _ = state.shape
    tiles = length // LANES

    def body(starts, flat, _, index, *refs):
        state, tail, work = refs[-3:]
        pack_stream(s, streams, tiles, flat, state.at[s], index, starts, work, tail.at[slot])

    given = [] if shared is None else [shared]
    return pl.pallas_call(
        body,
        in_specs=[IN_SMEM] + [IN_VMEM] * (3 + len(given)),
        out_specs=[IN_VMEM] * 2,
        out_shape=[
            pltpu.VMEM(state.shape, F32),
            pltpu.VMEM((number, features, SPAN), F32),
        ],
        scratch_shapes=[pltpu.VMEM((features, length + LANES), F32)],
        input_output_aliases={2: 0, **{4 + k: 1 for k in range(len(given))}},
        compiler_params=PARAMS,
        name="pack",
    )(starts, flat, state, index, *given)


def spread(s, at_stream, length, starts, arrived, state, ranks, lagging):
    streams, features, _ = state.shape

    def body(starts, arrived, _, ranks, *refs):
        *outs, joint, sent = refs[-4:] if s else (None,) + refs[-3:]
        state = outs[-2] if s else outs[-1]
        write = None
        if s:
            write = pltpu.make_async_copy(means_of(s - 1, length, state), outs[-1].at[s - 1], sent)
            write.start()
        spread_stream(s, at_stream, streams, length, starts, arrived, state, ranks, joint)
        if write is not None:
            write.wait()

    given = [] if lagging is None else [lagging]
    out_shape = [pltpu.VMEM(state.shape, F32)]
    if s:
        out_shape.append(jax.ShapeDtypeStruct((streams, features, length), F32))
    results = pl.pallas_call(
        body,
        in_specs=[IN_SMEM] + [IN_VMEM] * 3 + [IN_HBM] * len(given),
        out_specs=[IN_VMEM, IN_HBM][: len(out_shape)],
        out_shape=out_shape,
        scratch_shapes=[
            pltpu.VMEM((features, 2 * SPAN + LANES), F32),
            pltpu.SemaphoreType.DMA,
        ],
        input_output_aliases={2: 0, **{4 + k: 1 for k in range(len(given))}},
        compiler_params=PARAMS,
        name="spread",
    )(starts, arrived, state, ranks, *given)
    return (results[0], results[1] if s else None)


def between(chip, brought):
    counts = [len(brought[axis]) for axis in ROWS[:2]]

    def body(chip, *refs):
        *parts, out = refs
        out[...] = jnp.zeros(out.shape, F32)
        out[0:2, :] = chip[0:2, :]
        out[2:4, :] = earlier_rows(parts[: counts[0]], ROWS[0]) + earlier_rows(
            parts[counts[0] :], ROWS[1]
        )

    parts = [part for axis in ROWS[:2] for part in brought[axis]]
    return pl.pallas_call(
        body,
        in_specs=[IN_VMEM] * (1 + len(parts)),
        out_specs=IN_VMEM,
        out_shape=pltpu.VMEM((8, LANES), F32),
        compiler_params=PARAMS,
        name="between",
    )(chip, *parts)


def finish(length, state, ranks, lagging, own, core, rows):
    streams, features, _ = state.shape
    last = streams - 1
    tiles = length // LANES
    count = ranks.shape[0]

    def body(state, ranks, _, own, *refs):
        core_parts, row_parts = (refs[: len(core)], refs[len(core) : len(refs) - 7])
        lagging, deviation, columns, scale, staged, sent, gone = refs[-7:]
        writes = [
            pltpu.make_async_copy(means_of(last, length, state), lagging.at[last], sent)
        ]
        writes[0].start()
        before = own[2:4, :] + earlier_rows(core_parts, ROWS[3]) + earlier_rows(row_parts, ROWS[2])
        for part in row_parts:
            before = before + part[2:4, :]
        sums = before[0:1, :]
        row = lax.broadcasted_iota(I32, (features, LANES), 0)
        for s in range(streams):
            chosen = jnp.where(lanes_of(features) == row + s * features, sums, 0.0)
            columns[s] = jnp.broadcast_to(
                jnp.sum(chosen, axis=1, keepdims=True), (features, LANES)
            )
        stream = lax.broadcasted_iota(I32, (count, LANES), 0) & (streams - 1)
        seen = jnp.zeros((count, LANES), F32)
        for s in range(streams):
            tally = jnp.sum(jnp.where(lanes_of(1) == s, before[1:2, :], 0.0))
            seen = jnp.where(stream == s, tally, seen)
        scale[...] = 1.0 / jnp.maximum(seen + ranks[...].astype(F32), 1.0)
        for s in range(streams):
            column = columns[s]

            def step(g, carry, s=s, column=column):
                for j in range(GROUP):
                    t = g * GROUP + j
                    at = pl.multiple_of(t * LANES, LANES)
                    running = state[s, :, pl.ds(at, LANES)]
                    staged[s, :, pl.ds(at, LANES)] = state[s, :, pl.ds(length + at, LANES)] - (
                        column + running
                    ) * scale[pl.ds(t * streams + s, 1), :]
                return carry

            lax.fori_loop(0, tiles // GROUP, step, 0)
            write = pltpu.make_async_copy(staged.at[s], deviation.at[s], gone.at[s])
            write.start()
            writes.append(write)
        for write in writes:
            write.wait()

    shape = jax.ShapeDtypeStruct((streams, features, length), F32)
    return pl.pallas_call(
        body,
        in_specs=[IN_VMEM] * 2 + [IN_HBM] + [IN_VMEM] * (1 + len(core) + len(rows)),
        out_specs=[IN_HBM, IN_HBM],
        out_shape=[shape, shape],
        scratch_shapes=[
            pltpu.VMEM((streams, features, LANES), F32),
            pltpu.VMEM((count, LANES), F32),
            pltpu.VMEM((streams, features, length), F32),
            pltpu.SemaphoreType.DMA,
            pltpu.SemaphoreType.DMA((streams,)),
        ],
        input_output_aliases={2: 0},
        compiler_params=PARAMS,
        name="finish",
    )(state, ranks, lagging, own, *core, *rows)


def exchanged(totals, axis):
    count = lax.axis_size(axis)
    brought = []
    bit = 1
    while bit < count:
        other = lax.ppermute(totals, axis, [(k, k ^ (2 * bit - 1)) for k in range(count)])
        brought.append(other)
        totals = totals + other
        bit *= 2
    return brought, totals


def from_behind(value):
    count = lax.axis_size(ROWS)
    return lax.ppermute(value, ROWS, [(k, (k + 1) % count) for k in range(count)])


def per_device(events, keep):
    streams, _, length = events.shape
    state, flat, index, ranks, starts, tail, totals = pack_first(keep, events)
    arrived = [from_behind(tail)]
    for s in range(1, streams):
        state, tail = pack(s, length, starts, flat, state, index, 0, 1)
        arrived.append(from_behind(tail))
    brought = {}
    for axis in (ROWS[3], ROWS[1], ROWS[0]):
        brought[axis], totals = exchanged(totals, axis)
        if axis == ROWS[3]:
            chip = totals
    own = between(chip, brought)
    rows, _ = exchanged(own, ROWS[2])
    lagging = None
    for s in range(streams):
        state, lagging = spread(s, 0, length, starts, arrived[s], state, ranks, lagging)
    return tuple(
        finish(length, state, ranks, lagging, own, brought[ROWS[3]], rows)
    )


def solution(mesh):
    shape = SHAPE if mesh.size == 128 else (1, 1, mesh.size // 2, 2)
    finer = Mesh(mesh.devices.reshape(shape), ROWS)
    in_specs = (P(None, None, ROWS), P(None, ROWS))
    out_specs = (P(None, None, ROWS), P(None, None, ROWS))
    return jax.shard_map(
        per_device, mesh=finer, in_specs=in_specs, out_specs=out_specs, check_vma=False
    )
```

```python
import jax
import jax.numpy as jnp
from jax import lax
from jax.experimental import pallas as pl
from jax.experimental.pallas import tpu as pltpu
from jax.sharding import Mesh
from jax.sharding import PartitionSpec as P


SPAN = 4096
LANES = 128
GROUP = 64
GROUP_SUM = 16
ROWS = ("rows_0", "rows_1", "rows_2", "rows_3")
SHAPE = (4, 4, 4, 2)
F32 = jnp.float32
I32 = jnp.int32
BF16 = jnp.bfloat16


def lanes_of(rows):
    return lax.broadcasted_iota(I32, (rows, LANES), 1)


def picked_lanes(values, index):
    return jnp.take_along_axis(values, index, axis=1, mode="promise_in_bounds")


def running_weights():
    row = lax.broadcasted_iota(I32, (2 * LANES, 2 * LANES), 0) & (LANES - 1)
    column = lax.broadcasted_iota(I32, (2 * LANES, 2 * LANES), 1)
    return ((row <= column) | (column >= LANES)).astype(F32).astype(BF16)


def index_tables(keep, flat, scalars, copy, streams, tiles):
    count = streams * tiles
    for t in range(tiles):
        flat[t * streams : (t + 1) * streams, :] = keep[:, t * LANES : (t + 1) * LANES].astype(F32)
    flags = flat[...].astype(BF16)
    weights = running_weights()[:LANES]
    sums = jnp.dot(flags, weights, preferred_element_type=F32)
    within, total = (sums[:, :LANES], sums[:, LANES:])
    row = lax.broadcasted_iota(I32, (count, count), 0)
    column = lax.broadcasted_iota(I32, (count, count), 1)
    same = ((row ^ column) & (streams - 1)) == 0
    earlier = (same & (column < row)).astype(F32).astype(BF16)
    later = (same & (column > row)).astype(F32).astype(BF16)
    start = jnp.dot(earlier, total.astype(BF16), preferred_element_type=F32)
    line = lax.dot_general(
        jnp.ones((8, LANES), BF16), flags, (((1,), (1,)), ((), ())), preferred_element_type=F32
    )
    line_start = jnp.dot(line.astype(BF16), later, preferred_element_type=F32)
    sublane = lax.broadcasted_iota(I32, (8, count), 0)
    base = line_start + jnp.where(line == float(LANES), 1.0, 0.0)
    table = jnp.where(sublane == 0, line_start, jnp.where(sublane == 1, base, line_start + line))
    scalars[...] = table.astype(I32)
    copy.start()
    ordinal = lanes_of(count).astype(F32)
    place = jnp.zeros((count, LANES), I32)
    for step, times in ((32, 3), (8, 3), (2, 3), (1, 1)):
        found = place
        for k in range(1, times + 1):
            seen = picked_lanes(within, place + (k * step - 1))
            found = found + jnp.where(seen <= ordinal, step, 0)
        place = found
    begin = start.astype(I32)
    turned = picked_lanes(place, (lanes_of(count) - begin - 1) & (LANES - 1))
    return turned, begin + within.astype(I32)


def pack_stream(s, streams, tiles, flat, state, index, starts, work, tail):
    features = state.shape[0]
    lane = lanes_of(features)
    weights = running_weights()
    work[:, 0:LANES] = jnp.zeros((features, LANES), F32)

    def step(g, carry):
        tiles_in = []
        for j in range(GROUP):
            at = pl.multiple_of((g * GROUP + j) * LANES, LANES)
            kept = flat[pl.ds((g * GROUP + j) * streams + s, 1), :]
            tiles_in.append(state[:, pl.ds(at, LANES)] * kept)
        values = jnp.concatenate(tiles_in, axis=0)
        high = values.astype(BF16)
        low = (values - high.astype(F32)).astype(BF16)
        sums = jnp.dot(
            jnp.concatenate([high, low], axis=1), weights, preferred_element_type=F32
        )
        for j in range(GROUP):
            t = g * GROUP + j
            at = pl.multiple_of(t * LANES, LANES)
            block = sums[j * features : (j + 1) * features]
            running = carry + block[:, :LANES]
            carry = carry + block[:, LANES:]
            state[:, pl.ds(at, LANES)] = running
            order = jnp.broadcast_to(index[pl.ds(t * streams + s, 1), :], (features, LANES))
            packed = picked_lanes(running, order)
            slot = starts[0, t * streams + s] + 1
            low_at = pl.multiple_of((slot >> 7) * LANES, LANES)
            pltpu.store(
                work.at[:, pl.ds(low_at, LANES)], packed, mask=lane >= (slot & (LANES - 1))
            )
            work[:, pl.ds(low_at + LANES, LANES)] = packed
        return carry

    total = lax.fori_loop(0, tiles // GROUP, step, jnp.zeros((features, LANES), F32))
    state[:, tiles * LANES : tiles * LANES + SPAN + LANES] = work[:, : SPAN + LANES]
    first = starts[2, (tiles - 1) * streams + s] - SPAN
    tile, shift = (first >> 7, first & (LANES - 1))
    turn = (LANES - shift) & (LANES - 1)
    from_first = lane < LANES - shift

    def turned(m):
        at = pl.multiple_of((tile + m) * LANES, LANES)
        return pltpu.roll(work[:, pl.ds(at, LANES)], turn, 1)

    before = turned(0)
    for m in range(SPAN // LANES):
        after = turned(m + 1)
        tail[:, m * LANES : (m + 1) * LANES] = jnp.where(from_first, before, after) - total
        before = after
    return total


def totals_line(s, total):
    features = total.shape[0]
    row = lax.broadcasted_iota(I32, (features, LANES), 0)
    chosen = jnp.where(lanes_of(features) == row + s * features, total, 0.0)
    return jnp.sum(chosen, axis=0, keepdims=True)


def pack_first_body(
    keep_hbm, events, state, flat, index, ranks, starts, tail, totals,
    keep, scalars, work, copied, loaded,
):
    streams, length = keep.shape
    features = events.shape[1]
    tiles = length // LANES
    loads = [
        pltpu.make_async_copy(events.at[s], state.at[s, :, pl.ds(0, length)], loaded.at[s])
        for s in range(streams)
    ]
    flags = pltpu.make_async_copy(keep_hbm, keep, copied)
    flags.start()
    loads[0].start()
    flags.wait()
    for load in loads[1:]:
        load.start()
    copy = pltpu.make_async_copy(scalars, starts, copied)
    index[...], ranks[...] = index_tables(keep, flat, scalars, copy, streams, tiles)
    copy.wait()
    loads[0].wait()
    total = pack_stream(
        0, streams, tiles, flat, state.at[0], index, starts, work, tail.at[0]
    )
    for load in loads[1:]:
        load.wait()

    def step(g, sums):
        sums = list(sums)
        for j in range(GROUP_SUM):
            t = g * GROUP_SUM + j
            at = pl.multiple_of(t * LANES, LANES)
            for s in range(1, streams):
                kept = state[s, :, pl.ds(at, LANES)] * flat[pl.ds(t * streams + s, 1), :]
                sums[s - 1] = sums[s - 1] + kept
        return tuple(sums)

    zero = jnp.zeros((features, LANES), F32)
    sums = lax.fori_loop(0, tiles // GROUP_SUM, step, (zero,) * (streams - 1))
    sublane = lax.broadcasted_iota(I32, (8, LANES), 0)
    lane = lanes_of(8)
    counts = jnp.zeros((8, LANES), F32)
    for s in range(streams):
        counts = jnp.where(lane == s, starts[2, (tiles - 1) * streams + s].astype(F32), counts)
    line = totals_line(0, total)
    for s in range(1, streams):
        whole_sum = jnp.broadcast_to(
            jnp.sum(sums[s - 1], axis=1, keepdims=True), (features, LANES)
        )
        line = line + totals_line(s, whole_sum)
    line = jnp.broadcast_to(line, (8, LANES))
    totals[...] = jnp.where(sublane == 0, line, jnp.where(sublane == 1, counts, 0.0))


def spread_stream(s, at_stream, streams, length, starts, arrived, state, ranks, joint):
    features = state.shape[1]
    lane = lanes_of(features)
    joint[:, :SPAN] = jnp.where(lax.axis_index(ROWS) > 0, arrived[at_stream], 0.0)
    joint[:, SPAN:] = state[s, :, length : length + SPAN + LANES]

    def step(g, carry):
        for j in range(GROUP):
            t = g * GROUP + j
            row = t * streams + s
            at = pl.multiple_of(t * LANES, LANES)
            base = starts[1, row]
            low_at = pl.multiple_of((base >> 7) * LANES, LANES)
            window = jnp.where(
                lane >= (base & (LANES - 1)),
                joint[:, pl.ds(low_at, LANES)],
                joint[:, pl.ds(low_at + LANES, LANES)],
            )
            order = jnp.broadcast_to(ranks[pl.ds(row, 1), :] & (LANES - 1), (features, LANES))
            running = state[s, :, pl.ds(at, LANES)]
            state[s, :, pl.ds(length + at, LANES)] = (
                running - picked_lanes(window, order)
            ) * (1.0 / SPAN)
        return carry

    lax.fori_loop(0, length // LANES // GROUP, step, 0)


def means_of(s, length, state):
    return state.at[s, :, pl.ds(length, length)]


def taken(axis, bit):
    return ((lax.axis_index(axis) & bit) != 0).astype(F32)


def earlier_rows(brought, axis):
    number = len(brought)
    return sum(
        (brought[k][0:2, :] * taken(axis, 1 << k) for k in range(number)), jnp.zeros((2, LANES), F32)
    )


IN_VMEM = pl.BlockSpec(memory_space=pltpu.VMEM)
IN_SMEM = pl.BlockSpec(memory_space=pltpu.SMEM)
IN_HBM = pl.BlockSpec(memory_space=pltpu.HBM)
PARAMS = pltpu.CompilerParams(vmem_limit_bytes=12 << 20)


def pack_first(keep, events):
    streams, features, length = events.shape
    count = streams * length // LANES
    shapes = [
        pltpu.VMEM((streams, features, 2 * length), F32),
        pltpu.VMEM((count, LANES), F32),
        pltpu.VMEM((count, LANES), I32),
        pltpu.VMEM((count, LANES), I32),
        pltpu.SMEM((8, count), I32),
        pltpu.VMEM((1, features, SPAN), F32),
        pltpu.VMEM((8, LANES), F32),
    ]
    return pl.pallas_call(
        pack_first_body,
        in_specs=[IN_HBM, IN_HBM],
        out_specs=[IN_VMEM] * 4 + [IN_SMEM] + [IN_VMEM] * 2,
        out_shape=shapes,
        scratch_shapes=[
            pltpu.VMEM((streams, length), I32),
            pltpu.VMEM((8, count), I32),
            pltpu.VMEM((features, length + LANES), F32),
            pltpu.SemaphoreType.DMA,
            pltpu.SemaphoreType.DMA((streams,)),
        ],
        compiler_params=PARAMS,
        name="pack_first",
    )(
        pltpu.with_memory_space_constraint(keep, pltpu.HBM),
        pltpu.with_memory_space_constraint(events, pltpu.HBM),
    )


def pack(s, length, starts, flat, state, index, slot, number, shared=None):
    streams, features, _ = state.shape
    tiles = length // LANES

    def body(starts, flat, _, index, *refs):
        state, tail, work = refs[-3:]
        pack_stream(s, streams, tiles, flat, state.at[s], index, starts, work, tail.at[slot])

    given = [] if shared is None else [shared]
    return pl.pallas_call(
        body,
        in_specs=[IN_SMEM] + [IN_VMEM] * (3 + len(given)),
        out_specs=[IN_VMEM] * 2,
        out_shape=[
            pltpu.VMEM(state.shape, F32),
            pltpu.VMEM((number, features, SPAN), F32),
        ],
        scratch_shapes=[pltpu.VMEM((features, length + LANES), F32)],
        input_output_aliases={2: 0, **{4 + k: 1 for k in range(len(given))}},
        compiler_params=PARAMS,
        name="pack",
    )(starts, flat, state, index, *given)


def spread(s, at_stream, length, starts, arrived, state, ranks, lagging):
    streams, features, _ = state.shape

    def body(starts, arrived, _, ranks, *refs):
        *outs, joint, sent = refs[-4:] if s else (None,) + refs[-3:]
        state = outs[-2] if s else outs[-1]
        write = None
        if s:
            write = pltpu.make_async_copy(means_of(s - 1, length, state), outs[-1].at[s - 1], sent)
            write.start()
        spread_stream(s, at_stream, streams, length, starts, arrived, state, ranks, joint)
        if write is not None:
            write.wait()

    given = [] if lagging is None else [lagging]
    out_shape = [pltpu.VMEM(state.shape, F32)]
    if s:
        out_shape.append(jax.ShapeDtypeStruct((streams, features, length), F32))
    results = pl.pallas_call(
        body,
        in_specs=[IN_SMEM] + [IN_VMEM] * 3 + [IN_HBM] * len(given),
        out_specs=[IN_VMEM, IN_HBM][: len(out_shape)],
        out_shape=out_shape,
        scratch_shapes=[
            pltpu.VMEM((features, 2 * SPAN + LANES), F32),
            pltpu.SemaphoreType.DMA,
        ],
        input_output_aliases={2: 0, **{4 + k: 1 for k in range(len(given))}},
        compiler_params=PARAMS,
        name="spread",
    )(starts, arrived, state, ranks, *given)
    return (results[0], results[1] if s else None)


def between(chip, brought):
    counts = [len(brought[axis]) for axis in ROWS[:2]]

    def body(chip, *refs):
        *parts, out = refs
        out[...] = jnp.zeros(out.shape, F32)
        out[0:2, :] = chip[0:2, :]
        out[2:4, :] = earlier_rows(parts[: counts[0]], ROWS[0]) + earlier_rows(
            parts[counts[0] :], ROWS[1]
        )

    parts = [part for axis in ROWS[:2] for part in brought[axis]]
    return pl.pallas_call(
        body,
        in_specs=[IN_VMEM] * (1 + len(parts)),
        out_specs=IN_VMEM,
        out_shape=pltpu.VMEM((8, LANES), F32),
        compiler_params=PARAMS,
        name="between",
    )(chip, *parts)


def finish(length, state, ranks, lagging, own, core, rows):
    streams, features, _ = state.shape
    last = streams - 1
    tiles = length // LANES
    count = ranks.shape[0]

    def body(state, ranks, _, own, *refs):
        core_parts, row_parts = (refs[: len(core)], refs[len(core) : len(refs) - 7])
        lagging, deviation, columns, scale, staged, sent, gone = refs[-7:]
        writes = [
            pltpu.make_async_copy(means_of(last, length, state), lagging.at[last], sent)
        ]
        writes[0].start()
        before = own[2:4, :] + earlier_rows(core_parts, ROWS[3]) + earlier_rows(row_parts, ROWS[2])
        for part in row_parts:
            before = before + part[2:4, :]
        sums = before[0:1, :]
        row = lax.broadcasted_iota(I32, (features, LANES), 0)
        for s in range(streams):
            chosen = jnp.where(lanes_of(features) == row + s * features, sums, 0.0)
            columns[s] = jnp.broadcast_to(
                jnp.sum(chosen, axis=1, keepdims=True), (features, LANES)
            )
        stream = lax.broadcasted_iota(I32, (count, LANES), 0) & (streams - 1)
        seen = jnp.zeros((count, LANES), F32)
        for s in range(streams):
            tally = jnp.sum(jnp.where(lanes_of(1) == s, before[1:2, :], 0.0))
            seen = jnp.where(stream == s, tally, seen)
        scale[...] = 1.0 / jnp.maximum(seen + ranks[...].astype(F32), 1.0)
        for s in range(streams):
            column = columns[s]

            def step(g, carry, s=s, column=column):
                for j in range(GROUP):
                    t = g * GROUP + j
                    at = pl.multiple_of(t * LANES, LANES)
                    running = state[s, :, pl.ds(at, LANES)]
                    staged[s, :, pl.ds(at, LANES)] = state[s, :, pl.ds(length + at, LANES)] - (
                        column + running
                    ) * scale[pl.ds(t * streams + s, 1), :]
                return carry

            lax.fori_loop(0, tiles // GROUP, step, 0)
            write = pltpu.make_async_copy(staged.at[s], deviation.at[s], gone.at[s])
            write.start()
            writes.append(write)
        for write in writes:
            write.wait()

    shape = jax.ShapeDtypeStruct((streams, features, length), F32)
    return pl.pallas_call(
        body,
        in_specs=[IN_VMEM] * 2 + [IN_HBM] + [IN_VMEM] * (1 + len(core) + len(rows)),
        out_specs=[IN_HBM, IN_HBM],
        out_shape=[shape, shape],
        scratch_shapes=[
            pltpu.VMEM((streams, features, LANES), F32),
            pltpu.VMEM((count, LANES), F32),
            pltpu.VMEM((streams, features, length), F32),
            pltpu.SemaphoreType.DMA,
            pltpu.SemaphoreType.DMA((streams,)),
        ],
        input_output_aliases={2: 0},
        compiler_params=PARAMS,
        name="finish",
    )(state, ranks, lagging, own, *core, *rows)


def exchanged(totals, axis):
    count = lax.axis_size(axis)
    brought = []
    bit = 1
    while bit < count:
        other = lax.ppermute(totals, axis, [(k, k ^ (2 * bit - 1)) for k in range(count)])
        brought.append(other)
        totals = totals + other
        bit *= 2
    return brought, totals


def from_behind(value):
    count = lax.axis_size(ROWS)
    return lax.ppermute(value, ROWS, [(k, (k + 1) % count) for k in range(count)])


def per_device(events, keep):
    streams, _, length = events.shape
    state, flat, index, ranks, starts, tail, totals = pack_first(keep, events)
    arrived = [from_behind(tail)]
    for s in range(1, streams):
        state, tail = pack(s, length, starts, flat, state, index, 0, 1)
        arrived.append(from_behind(tail))
    brought = {}
    for axis in (ROWS[3], ROWS[1], ROWS[0]):
        brought[axis], totals = exchanged(totals, axis)
        if axis == ROWS[3]:
            chip = totals
    own = between(chip, brought)
    rows, _ = exchanged(own, ROWS[2])
    lagging = None
    for s in range(streams):
        state, lagging = spread(s, 0, length, starts, arrived[s], state, ranks, lagging)
    return tuple(
        finish(length, state, ranks, lagging, own, brought[ROWS[3]], rows)
    )


def solution(mesh):
    shape = SHAPE if mesh.size == 128 else (1, 1, mesh.size // 2, 2)
    finer = Mesh(mesh.devices.reshape(shape), ROWS)
    in_specs = (P(None, None, ROWS), P(None, ROWS))
    out_specs = (P(None, None, ROWS), P(None, None, ROWS))
    return jax.shard_map(
        per_device, mesh=finer, in_specs=in_specs, out_specs=out_specs, check_vma=False
    )
```

```python
import itertools

import jax
import jax.numpy as jnp
from jax import lax
from jax.experimental import pallas as pl
from jax.experimental.pallas import tpu as pltpu
from jax.sharding import Mesh
from jax.sharding import PartitionSpec as P


SPAN = 4096
LANES = 128
GROUP = 64
GROUP_SUM = 16
PARTS = 2
ROWS = ("rows_0", "rows_1", "rows_2", "rows_3")
SHAPE = (4, 4, 4, 2)
F32 = jnp.float32
I32 = jnp.int32
BF16 = jnp.bfloat16


def lanes_of(rows):
    return lax.broadcasted_iota(I32, (rows, LANES), 1)


def picked_lanes(values, index):
    return jnp.take_along_axis(values, index, axis=1, mode="promise_in_bounds")


def running_weights():
    row = lax.broadcasted_iota(I32, (2 * LANES, 2 * LANES), 0) & (LANES - 1)
    column = lax.broadcasted_iota(I32, (2 * LANES, 2 * LANES), 1)
    return ((row <= column) | (column >= LANES)).astype(F32).astype(BF16)


def index_tables(keep, flat, scalars, copy, streams, tiles):
    count = streams * tiles
    for t in range(tiles):
        flat[t * streams : (t + 1) * streams, :] = keep[:, t * LANES : (t + 1) * LANES].astype(F32)
    flags = flat[...].astype(BF16)
    weights = running_weights()[:LANES]
    sums = jnp.dot(flags, weights, preferred_element_type=F32)
    within, total = (sums[:, :LANES], sums[:, LANES:])
    row = lax.broadcasted_iota(I32, (count, count), 0)
    column = lax.broadcasted_iota(I32, (count, count), 1)
    same = ((row ^ column) & (streams - 1)) == 0
    earlier = (same & (column < row)).astype(F32).astype(BF16)
    later = (same & (column > row)).astype(F32).astype(BF16)
    start = jnp.dot(earlier, total.astype(BF16), preferred_element_type=F32)
    line = lax.dot_general(
        jnp.ones((8, LANES), BF16), flags, (((1,), (1,)), ((), ())), preferred_element_type=F32
    )
    line_start = jnp.dot(line.astype(BF16), later, preferred_element_type=F32)
    sublane = lax.broadcasted_iota(I32, (8, count), 0)
    base = line_start + jnp.where(line == float(LANES), 1.0, 0.0)
    table = jnp.where(sublane == 0, line_start, jnp.where(sublane == 1, base, line_start + line))
    scalars[...] = table.astype(I32)
    copy.start()
    ordinal = lanes_of(count).astype(F32)
    place = jnp.zeros((count, LANES), I32)
    for step, times in ((32, 3), (8, 3), (2, 3), (1, 1)):
        found = place
        for k in range(1, times + 1):
            seen = picked_lanes(within, place + (k * step - 1))
            found = found + jnp.where(seen <= ordinal, step, 0)
        place = found
    begin = start.astype(I32)
    turned = picked_lanes(place, (lanes_of(count) - begin - 1) & (LANES - 1))
    return turned, begin + within.astype(I32)


def pack_stream(s, streams, tiles, flat, state, index, starts, work, tail):
    features = state.shape[0]
    lane = lanes_of(features)
    weights = running_weights()
    work[:, 0:LANES] = jnp.zeros((features, LANES), F32)

    def step(g, carry):
        tiles_in = []
        for j in range(GROUP):
            at = pl.multiple_of((g * GROUP + j) * LANES, LANES)
            kept = flat[pl.ds((g * GROUP + j) * streams + s, 1), :]
            tiles_in.append(state[:, pl.ds(at, LANES)] * kept)
        values = jnp.concatenate(tiles_in, axis=0)
        high = values.astype(BF16)
        low = (values - high.astype(F32)).astype(BF16)
        sums = jnp.dot(
            jnp.concatenate([high, low], axis=1), weights, preferred_element_type=F32
        )
        for j in range(GROUP):
            t = g * GROUP + j
            at = pl.multiple_of(t * LANES, LANES)
            block = sums[j * features : (j + 1) * features]
            running = carry + block[:, :LANES]
            carry = carry + block[:, LANES:]
            state[:, pl.ds(at, LANES)] = running
            order = jnp.broadcast_to(index[pl.ds(t * streams + s, 1), :], (features, LANES))
            packed = picked_lanes(running, order)
            slot = starts[0, t * streams + s] + 1
            low_at = pl.multiple_of((slot >> 7) * LANES, LANES)
            pltpu.store(
                work.at[:, pl.ds(low_at, LANES)], packed, mask=lane >= (slot & (LANES - 1))
            )
            work[:, pl.ds(low_at + LANES, LANES)] = packed
        return carry

    total = lax.fori_loop(0, tiles // GROUP, step, jnp.zeros((features, LANES), F32))
    state[:, tiles * LANES : tiles * LANES + SPAN + LANES] = work[:, : SPAN + LANES]
    first = starts[2, (tiles - 1) * streams + s] - SPAN
    tile, shift = (first >> 7, first & (LANES - 1))
    turn = (LANES - shift) & (LANES - 1)
    from_first = lane < LANES - shift

    def turned(m):
        at = pl.multiple_of((tile + m) * LANES, LANES)
        return pltpu.roll(work[:, pl.ds(at, LANES)], turn, 1)

    before = turned(0)
    for m in range(SPAN // LANES):
        after = turned(m + 1)
        tail[:, m * LANES : (m + 1) * LANES] = jnp.where(from_first, before, after) - total
        before = after
    return total


def totals_line(s, total):
    features = total.shape[0]
    row = lax.broadcasted_iota(I32, (features, LANES), 0)
    chosen = jnp.where(lanes_of(features) == row + s * features, total, 0.0)
    return jnp.sum(chosen, axis=0, keepdims=True)


def pack_first_body(
    keep_hbm, events, state, flat, index, ranks, starts, tail, totals,
    keep, scalars, work, copied, loaded,
):
    streams, length = keep.shape
    tiles = length // LANES
    loads = [
        pltpu.make_async_copy(events.at[s], state.at[s, :, pl.ds(0, length)], loaded.at[s])
        for s in range(streams)
    ]
    flags = pltpu.make_async_copy(keep_hbm, keep, copied)
    flags.start()
    loads[0].start()
    flags.wait()
    for load in loads[1:]:
        load.start()
    copy = pltpu.make_async_copy(scalars, starts, copied)
    index[...], ranks[...] = index_tables(keep, flat, scalars, copy, streams, tiles)
    copy.wait()
    loads[0].wait()
    total = pack_stream(
        0, streams, tiles, flat, state.at[0], index, starts, work, tail.at[0]
    )
    for load in loads[1:]:
        load.wait()

    sublane = lax.broadcasted_iota(I32, (8, LANES), 0)
    lane = lanes_of(8)
    counts = jnp.zeros((8, LANES), F32)
    for s in range(streams):
        counts = jnp.where(lane == s, starts[2, (tiles - 1) * streams + s].astype(F32), counts)
    line = jnp.broadcast_to(totals_line(0, total), (8, LANES))
    totals[...] = jnp.where(sublane == 0, line, jnp.where(sublane == 1, counts, 0.0))


def joined(s, length, arrived, state, joint):
    joint[:, :SPAN] = jnp.where(lax.axis_index(ROWS) > 0, arrived[0], 0.0)
    joint[:, SPAN:] = state[s, :, length : length + SPAN + LANES]


def window_mean(s, t, streams, starts, state, ranks, joint):
    features = state.shape[1]
    row = t * streams + s
    base = starts[1, row]
    low_at = pl.multiple_of((base >> 7) * LANES, LANES)
    window = jnp.where(
        lanes_of(features) >= (base & (LANES - 1)),
        joint[:, pl.ds(low_at, LANES)],
        joint[:, pl.ds(low_at + LANES, LANES)],
    )
    order = jnp.broadcast_to(ranks[row : row + 1, :] & (LANES - 1), (features, LANES))
    running = state[s, :, t * LANES : (t + 1) * LANES]
    return running, (running - picked_lanes(window, order)) * (1.0 / SPAN)


def means_of(s, length, state):
    return state.at[s, :, pl.ds(length, length)]


def taken(axis, bit):
    return ((lax.axis_index(axis) & bit) != 0).astype(F32)


def earlier_rows(brought, axis):
    number = len(brought)
    return sum(
        (brought[k][0:2, :] * taken(axis, 1 << k) for k in range(number)), jnp.zeros((2, LANES), F32)
    )


IN_VMEM = pl.BlockSpec(memory_space=pltpu.VMEM)
IN_SMEM = pl.BlockSpec(memory_space=pltpu.SMEM)
IN_HBM = pl.BlockSpec(memory_space=pltpu.HBM)
PARAMS = pltpu.CompilerParams(vmem_limit_bytes=12 << 20)


def pack_first(keep, events):
    streams, features, length = events.shape
    count = streams * length // LANES
    shapes = [
        pltpu.VMEM((streams, features, 2 * length), F32),
        pltpu.VMEM((count, LANES), F32),
        pltpu.VMEM((count, LANES), I32),
        pltpu.VMEM((count, LANES), I32),
        pltpu.SMEM((8, count), I32),
        pltpu.VMEM((1, features, SPAN), F32),
        pltpu.VMEM((8, LANES), F32),
    ]
    return pl.pallas_call(
        pack_first_body,
        in_specs=[IN_HBM, IN_HBM],
        out_specs=[IN_VMEM] * 4 + [IN_SMEM] + [IN_VMEM] * 2,
        out_shape=shapes,
        scratch_shapes=[
            pltpu.VMEM((streams, length), I32),
            pltpu.VMEM((8, count), I32),
            pltpu.VMEM((features, length + LANES), F32),
            pltpu.SemaphoreType.DMA,
            pltpu.SemaphoreType.DMA((streams,)),
        ],
        compiler_params=PARAMS,
        name="pack_first",
    )(
        pltpu.with_memory_space_constraint(keep, pltpu.HBM),
        pltpu.with_memory_space_constraint(events, pltpu.HBM),
    )


def pack(s, length, starts, flat, state, index, slot, number, shared=None):
    streams, features, _ = state.shape
    tiles = length // LANES

    def body(starts, flat, _, index, *refs):
        state, tail, work = refs[-3:]
        pack_stream(s, streams, tiles, flat, state.at[s], index, starts, work, tail.at[slot])

    given = [] if shared is None else [shared]
    return pl.pallas_call(
        body,
        in_specs=[IN_SMEM] + [IN_VMEM] * (3 + len(given)),
        out_specs=[IN_VMEM] * 2,
        out_shape=[
            pltpu.VMEM(state.shape, F32),
            pltpu.VMEM((number, features, SPAN), F32),
        ],
        scratch_shapes=[pltpu.VMEM((features, length + LANES), F32)],
        input_output_aliases={2: 0, **{4 + k: 1 for k in range(len(given))}},
        compiler_params=PARAMS,
        name="pack",
    )(starts, flat, state, index, *given)


def add_totals(length, flat, state, totals):
    streams, features, _ = state.shape
    tiles = length // LANES

    def body(flat, _, so_far, state, totals):
        def step(g, sums):
            sums = list(sums)
            for j in range(GROUP_SUM):
                t = g * GROUP_SUM + j
                at = pl.multiple_of(t * LANES, LANES)
                for s in range(1, streams):
                    kept = state[s, :, pl.ds(at, LANES)] * flat[pl.ds(t * streams + s, 1), :]
                    sums[s - 1] = sums[s - 1] + kept
            return tuple(sums)

        zero = jnp.zeros((features, LANES), F32)
        sums = lax.fori_loop(0, tiles // GROUP_SUM, step, (zero,) * (streams - 1))
        line = jnp.zeros((1, LANES), F32)
        for s in range(1, streams):
            whole_sum = jnp.broadcast_to(
                jnp.sum(sums[s - 1], axis=1, keepdims=True), (features, LANES)
            )
            line = line + totals_line(s, whole_sum)
        sublane = lax.broadcasted_iota(I32, (8, LANES), 0)
        line = jnp.broadcast_to(line, (8, LANES))
        totals[...] = so_far[...] + jnp.where(sublane == 0, line, 0.0)

    return pl.pallas_call(
        body,
        in_specs=[IN_VMEM] * 3,
        out_specs=[IN_VMEM] * 2,
        out_shape=[pltpu.VMEM(state.shape, F32), pltpu.VMEM((8, LANES), F32)],
        input_output_aliases={1: 0},
        compiler_params=PARAMS,
        name="add_totals",
    )(flat, state, totals)


def spread(s, length, starts, arrived, state, ranks, lagging):
    streams, features, _ = state.shape

    def body(starts, arrived, _, ranks, *refs):
        *outs, joint, sent = refs[-4:] if s else (None,) + refs[-3:]
        state = outs[-2] if s else outs[-1]
        write = None
        if s:
            write = pltpu.make_async_copy(means_of(s - 1, length, state), outs[-1].at[s - 1], sent)
            write.start()
        joined(s, length, arrived, state, joint)
        for t in range(length // LANES):
            _, mean = window_mean(s, t, streams, starts, state, ranks, joint)
            state[s, :, length + t * LANES : length + (t + 1) * LANES] = mean
        if write is not None:
            write.wait()

    given = [] if lagging is None else [lagging]
    out_shape = [pltpu.VMEM(state.shape, F32)]
    if s:
        out_shape.append(jax.ShapeDtypeStruct((streams, features, length), F32))
    results = pl.pallas_call(
        body,
        in_specs=[IN_SMEM] + [IN_VMEM] * 3 + [IN_HBM] * len(given),
        out_specs=[IN_VMEM, IN_HBM][: len(out_shape)],
        out_shape=out_shape,
        scratch_shapes=[
            pltpu.VMEM((features, 2 * SPAN + LANES), F32),
            pltpu.SemaphoreType.DMA,
        ],
        input_output_aliases={2: 0, **{4 + k: 1 for k in range(len(given))}},
        compiler_params=PARAMS,
        name="spread",
    )(starts, arrived, state, ranks, *given)
    return (results[0], results[1] if s else None)


def between(chip, brought):
    counts = [len(brought[axis]) for axis in ROWS[:2]]

    def body(chip, *refs):
        *parts, out = refs
        out[...] = jnp.zeros(out.shape, F32)
        out[0:2, :] = chip[0:2, :]
        out[2:4, :] = earlier_rows(parts[: counts[0]], ROWS[0]) + earlier_rows(
            parts[counts[0] :], ROWS[1]
        )

    parts = [part for axis in ROWS[:2] for part in brought[axis]]
    return pl.pallas_call(
        body,
        in_specs=[IN_VMEM] * (1 + len(parts)),
        out_specs=IN_VMEM,
        out_shape=pltpu.VMEM((8, LANES), F32),
        compiler_params=PARAMS,
        name="between",
    )(chip, *parts)


def deviate(length, state, ranks, lagging, own, core, rows, sides):
    streams, features, _ = state.shape
    last = streams - 1
    tiles = length // LANES
    count = ranks.shape[0]

    def body(state, ranks, _, own, *refs):
        core_parts, row_parts = (refs[: len(core)], refs[len(core) : len(refs) - 7])
        at_core = lax.axis_index(ROWS[3])
        row_parts = [
            jnp.where(at_core == sides[k], row_parts[2 * k][0:4, :], row_parts[2 * k + 1][0:4, :])
            for k in range(len(sides))
        ]
        lagging, deviation, columns, scale, staged, sent, gone = refs[-7:]
        writes = [
            pltpu.make_async_copy(means_of(last - 1, length, state), lagging.at[last - 1], sent)
        ]
        writes[0].start()
        before = own[2:4, :] + earlier_rows(core_parts, ROWS[3]) + earlier_rows(row_parts, ROWS[2])
        for part in row_parts:
            before = before + part[2:4, :]
        sums = before[0:1, :]
        row = lax.broadcasted_iota(I32, (features, LANES), 0)
        for s in range(streams):
            chosen = jnp.where(lanes_of(features) == row + s * features, sums, 0.0)
            columns[s] = jnp.broadcast_to(
                jnp.sum(chosen, axis=1, keepdims=True), (features, LANES)
            )
        stream = lax.broadcasted_iota(I32, (count, LANES), 0) & (streams - 1)
        seen = jnp.zeros((count, LANES), F32)
        for s in range(streams):
            tally = jnp.sum(jnp.where(lanes_of(1) == s, before[1:2, :], 0.0))
            seen = jnp.where(stream == s, tally, seen)
        scale[...] = 1.0 / jnp.maximum(seen + ranks[...].astype(F32), 1.0)
        for s in range(last):
            column = columns[s]
            for t in range(tiles):
                at = slice(t * LANES, (t + 1) * LANES)
                mean = state[s, :, length + t * LANES : length + (t + 1) * LANES]
                staged[s, :, at] = mean - (column + state[s, :, at]) * scale[
                    t * streams + s : t * streams + s + 1, :
                ]
            write = pltpu.make_async_copy(staged.at[s], deviation.at[s], gone.at[s])
            write.start()
            writes.append(write)
        for write in writes:
            write.wait()

    shape = jax.ShapeDtypeStruct((streams, features, length), F32)
    return pl.pallas_call(
        body,
        in_specs=[IN_VMEM] * 2 + [IN_HBM] + [IN_VMEM] * (1 + len(core) + len(rows)),
        out_specs=[IN_HBM, IN_HBM, IN_VMEM, IN_VMEM],
        out_shape=[
            shape,
            shape,
            pltpu.VMEM((streams, features, LANES), F32),
            pltpu.VMEM((count, LANES), F32),
        ],
        scratch_shapes=[
            pltpu.VMEM((last, features, length), F32),
            pltpu.SemaphoreType.DMA,
            pltpu.SemaphoreType.DMA((last,)),
        ],
        input_output_aliases={2: 0},
        compiler_params=PARAMS,
        name="deviate",
    )(state, ranks, lagging, own, *core, *rows)


def finish(length, starts, arrived, state, ranks, columns, scale, outputs):
    streams, features, _ = state.shape
    s = streams - 1
    tiles = length // LANES

    def body(starts, arrived, state, ranks, columns, scale, *refs):
        lagging, deviation, joint, means, deviations, sent, gone = refs[-7:]
        joined(s, length, arrived, state, joint)
        column = columns[s]
        writes = []
        for part in range(PARTS):
            for t in range(part * tiles // PARTS, (part + 1) * tiles // PARTS):
                at = slice(t * LANES, (t + 1) * LANES)
                running, mean = window_mean(s, t, streams, starts, state, ranks, joint)
                means[:, at] = mean
                deviations[:, at] = mean - (column + running) * scale[
                    t * streams + s : t * streams + s + 1, :
                ]
            at = pl.ds(part * length // PARTS, length // PARTS)
            for source, target, done in ((means, lagging, sent), (deviations, deviation, gone)):
                writes.append(
                    pltpu.make_async_copy(source.at[:, at], target.at[s, :, at], done.at[part])
                )
                writes[-1].start()
        for write in writes:
            write.wait()

    return pl.pallas_call(
        body,
        in_specs=[IN_SMEM] + [IN_VMEM] * 5 + [IN_HBM] * 2,
        out_specs=[IN_HBM] * 2,
        out_shape=[jax.ShapeDtypeStruct((streams, features, length), F32)] * 2,
        scratch_shapes=[
            pltpu.VMEM((features, 2 * SPAN + LANES), F32),
            pltpu.VMEM((features, length), F32),
            pltpu.VMEM((features, length), F32),
            pltpu.SemaphoreType.DMA((PARTS,)),
            pltpu.SemaphoreType.DMA((PARTS,)),
        ],
        input_output_aliases={6: 0, 7: 1},
        compiler_params=PARAMS,
        name="finish",
    )(starts, arrived, state, ranks, columns, scale, *outputs)


def permuted(value, target):
    places = list(itertools.product(*(range(lax.axis_size(axis)) for axis in ROWS)))
    number = {place: k for k, place in enumerate(places)}
    return lax.ppermute(
        value, ROWS, [(number[place], number[target(*place)]) for place in places]
    )


def exchanged(totals, axis):
    count = lax.axis_size(axis)
    brought = []
    bit = 1
    while bit < count:
        flip = 2 * bit - 1

        def target(z, y, x, core, flip=flip):
            return (z ^ flip, y, x, 1 - core) if axis == ROWS[0] else (z, y ^ flip, x, 1 - core)

        other = permuted(totals, target)
        brought.append(other)
        totals = totals + other
        bit *= 2
    return brought, totals


def other_core(value):
    return permuted(value, lambda z, y, x, core: (z, y, x, 1 - core))


def exchanged_rows(totals):
    count = lax.axis_size(ROWS[2])
    brought, sides = ([], [])
    bit = 1
    while bit < count:
        flip, side = (2 * bit - 1, int(2 * bit >= count))

        def target(z, y, x, core, flip=flip, side=side):
            return (z, y, (x - 1) % count, 1 - side) if core else (z, y, x ^ flip, side)

        other = permuted(totals, target)
        brought += [other, other_core(other)]
        sides.append(side)
        totals = totals + other
        bit *= 2
    return brought, sides


def from_behind(value):
    count = lax.axis_size(ROWS)
    return lax.ppermute(value, ROWS, [(k, (k + 1) % count) for k in range(count)])


def per_device(events, keep):
    streams, _, length = events.shape
    state, flat, index, ranks, starts, tail, totals = pack_first(keep, events)
    arrived = [from_behind(tail)]
    state, totals = add_totals(length, flat, state, totals)
    for s in range(1, streams):
        state, tail = pack(s, length, starts, flat, state, index, 0, 1)
        arrived.append(from_behind(tail))
    brought = {ROWS[3]: [other_core(totals)]}
    chip = totals = totals + brought[ROWS[3]][0]
    for axis in (ROWS[1], ROWS[0]):
        brought[axis], totals = exchanged(totals, axis)
    own = between(chip, brought)
    rows, sides = exchanged_rows(own)
    lagging = None
    for s in range(streams - 1):
        state, lagging = spread(s, length, starts, arrived[s], state, ranks, lagging)
    *outputs, columns, scale = deviate(
        length, state, ranks, lagging, own, brought[ROWS[3]], rows, sides
    )
    return tuple(
        finish(length, starts, arrived[-1], state, ranks, columns, scale, outputs)
    )


def solution(mesh):
    shape = SHAPE if mesh.size == 128 else (1, 1, mesh.size // 2, 2)
    finer = Mesh(mesh.devices.reshape(shape), ROWS)
    in_specs = (P(None, None, ROWS), P(None, ROWS))
    out_specs = (P(None, None, ROWS), P(None, None, ROWS))
    return jax.shard_map(
        per_device, mesh=finer, in_specs=in_specs, out_specs=out_specs, check_vma=False
    )
```

```python
import itertools

import jax
import jax.numpy as jnp
from jax import lax
from jax.experimental import pallas as pl
from jax.experimental.pallas import tpu as pltpu
from jax.sharding import Mesh
from jax.sharding import PartitionSpec as P


SPAN = 4096
LANES = 128
GROUP = 64
GROUP_SUM = 16
PARTS = 4
ROWS = ("rows_0", "rows_1", "rows_2", "rows_3")
SHAPE = (4, 4, 4, 2)
F32 = jnp.float32
I32 = jnp.int32
BF16 = jnp.bfloat16


def lanes_of(rows):
    return lax.broadcasted_iota(I32, (rows, LANES), 1)


def picked_lanes(values, index):
    return jnp.take_along_axis(values, index, axis=1, mode="promise_in_bounds")


def running_weights():
    row = lax.broadcasted_iota(I32, (2 * LANES, 2 * LANES), 0) & (LANES - 1)
    column = lax.broadcasted_iota(I32, (2 * LANES, 2 * LANES), 1)
    return ((row <= column) | (column >= LANES)).astype(F32).astype(BF16)


def index_tables(keep, flags_in, loads, masks, flat, scalars, copy, streams, tiles):
    count = streams * tiles
    row = lax.broadcasted_iota(I32, (count, count), 0)
    column = lax.broadcasted_iota(I32, (count, count), 1)
    same = ((row ^ column) & (streams - 1)) == 0
    masks[0] = (same & (column < row)).astype(F32).astype(BF16)
    masks[1] = (same & (column > row)).astype(F32).astype(BF16)
    flags_in.wait()
    for load in loads:
        load.start()
    for t in range(tiles):
        flat[t * streams : (t + 1) * streams, :] = keep[:, t * LANES : (t + 1) * LANES].astype(F32)
    flags = flat[...].astype(BF16)
    weights = running_weights()[:LANES]
    sums = jnp.dot(flags, weights, preferred_element_type=F32)
    within, total = (sums[:, :LANES], sums[:, LANES:])
    start = jnp.dot(masks[0], total.astype(BF16), preferred_element_type=F32)
    line = lax.dot_general(
        jnp.ones((8, LANES), BF16), flags, (((1,), (1,)), ((), ())), preferred_element_type=F32
    )
    line_start = jnp.dot(line.astype(BF16), masks[1], preferred_element_type=F32)
    sublane = lax.broadcasted_iota(I32, (8, count), 0)
    base = line_start + jnp.where(line == float(LANES), 1.0, 0.0)
    table = jnp.where(sublane == 0, line_start, jnp.where(sublane == 1, base, line_start + line))
    scalars[...] = table.astype(I32)
    copy.start()
    ordinal = lanes_of(count).astype(F32)
    place = jnp.zeros((count, LANES), I32)
    for step, times in ((64, 1), (32, 1), (16, 1), (8, 1), (4, 1), (2, 1), (1, 1)):
        found = place
        for k in range(1, times + 1):
            seen = picked_lanes(within, place + (k * step - 1))
            found = found + jnp.where(seen <= ordinal, step, 0)
        place = found
    begin = start.astype(I32)
    turned = picked_lanes(place, (lanes_of(count) - begin - 1) & (LANES - 1))
    return turned, begin + within.astype(I32)


def pack_stream(s, streams, tiles, flat, state, index, starts, work, tail):
    features = state.shape[0]
    lane = lanes_of(features)
    weights = running_weights()
    work[:, 0:LANES] = jnp.zeros((features, LANES), F32)

    def step(g, carry):
        tiles_in = []
        for j in range(GROUP):
            at = pl.multiple_of((g * GROUP + j) * LANES, LANES)
            kept = flat[pl.ds((g * GROUP + j) * streams + s, 1), :]
            tiles_in.append(state[:, pl.ds(at, LANES)] * kept)
        values = jnp.concatenate(tiles_in, axis=0)
        high = values.astype(BF16)
        low = (values - high.astype(F32)).astype(BF16)
        sums = jnp.dot(
            jnp.concatenate([high, low], axis=1), weights, preferred_element_type=F32
        )
        for j in range(GROUP):
            t = g * GROUP + j
            at = pl.multiple_of(t * LANES, LANES)
            block = sums[j * features : (j + 1) * features]
            running = carry + block[:, :LANES]
            carry = carry + block[:, LANES:]
            state[:, pl.ds(at, LANES)] = running
            order = jnp.broadcast_to(index[pl.ds(t * streams + s, 1), :], (features, LANES))
            packed = picked_lanes(running, order)
            slot = starts[0, t * streams + s] + 1
            low_at = pl.multiple_of((slot >> 7) * LANES, LANES)
            pltpu.store(
                work.at[:, pl.ds(low_at, LANES)], packed, mask=lane >= (slot & (LANES - 1))
            )
            work[:, pl.ds(low_at + LANES, LANES)] = packed
        return carry

    total = lax.fori_loop(0, tiles // GROUP, step, jnp.zeros((features, LANES), F32))
    state[:, tiles * LANES : tiles * LANES + SPAN + LANES] = work[:, : SPAN + LANES]
    first = starts[2, (tiles - 1) * streams + s] - SPAN
    tile, shift = (first >> 7, first & (LANES - 1))
    turn = (LANES - shift) & (LANES - 1)
    from_first = lane < LANES - shift

    def turned(m):
        at = pl.multiple_of((tile + m) * LANES, LANES)
        return pltpu.roll(work[:, pl.ds(at, LANES)], turn, 1)

    before = turned(0)
    for m in range(SPAN // LANES):
        after = turned(m + 1)
        tail[:, m * LANES : (m + 1) * LANES] = jnp.where(from_first, before, after) - total
        before = after
    return total


def totals_line(s, total):
    features = total.shape[0]
    row = lax.broadcasted_iota(I32, (features, LANES), 0)
    chosen = jnp.where(lanes_of(features) == row + s * features, total, 0.0)
    return jnp.sum(chosen, axis=0, keepdims=True)


def pack_first_body(
    keep_hbm, events, state, flat, index, ranks, starts, tail, totals,
    keep, scalars, masks, work, copied, published, loaded,
):
    streams, length = keep.shape
    tiles = length // LANES
    loads = [
        pltpu.make_async_copy(events.at[s], state.at[s, :, pl.ds(0, length)], loaded.at[s])
        for s in range(streams)
    ]
    flags = pltpu.make_async_copy(keep_hbm, keep, copied)
    flags.start()
    loads[0].start()
    copy = pltpu.make_async_copy(scalars, starts, published)
    index[...], ranks[...] = index_tables(
        keep, flags, loads[1:], masks, flat, scalars, copy, streams, tiles
    )
    copy.wait()
    loads[0].wait()
    total = pack_stream(
        0, streams, tiles, flat, state.at[0], index, starts, work, tail.at[0]
    )
    for load in loads[1:]:
        load.wait()

    sublane = lax.broadcasted_iota(I32, (8, LANES), 0)
    lane = lanes_of(8)
    counts = jnp.zeros((8, LANES), F32)
    for s in range(streams):
        counts = jnp.where(lane == s, starts[2, (tiles - 1) * streams + s].astype(F32), counts)
    line = jnp.broadcast_to(totals_line(0, total), (8, LANES))
    totals[...] = jnp.where(sublane == 0, line, jnp.where(sublane == 1, counts, 0.0))


def joined(s, length, arrived, state, joint):
    joint[:, :SPAN] = jnp.where(lax.axis_index(ROWS) > 0, arrived[0], 0.0)
    joint[:, SPAN:] = state[s, :, length : length + SPAN + LANES]


def window_mean(s, t, streams, starts, state, ranks, joint):
    features = state.shape[1]
    row = t * streams + s
    base = starts[1, row]
    low_at = pl.multiple_of((base >> 7) * LANES, LANES)
    window = jnp.where(
        lanes_of(features) >= (base & (LANES - 1)),
        joint[:, pl.ds(low_at, LANES)],
        joint[:, pl.ds(low_at + LANES, LANES)],
    )
    order = jnp.broadcast_to(ranks[row : row + 1, :] & (LANES - 1), (features, LANES))
    running = state[s, :, t * LANES : (t + 1) * LANES]
    return running, (running - picked_lanes(window, order)) * (1.0 / SPAN)


def means_of(s, length, state):
    return state.at[s, :, pl.ds(length, length)]


def taken(axis, bit):
    return ((lax.axis_index(axis) & bit) != 0).astype(F32)


def earlier_rows(brought, axis):
    number = len(brought)
    return sum(
        (brought[k][0:2, :] * taken(axis, 1 << k) for k in range(number)), jnp.zeros((2, LANES), F32)
    )


IN_VMEM = pl.BlockSpec(memory_space=pltpu.VMEM)
IN_SMEM = pl.BlockSpec(memory_space=pltpu.SMEM)
IN_HBM = pl.BlockSpec(memory_space=pltpu.HBM)
PARAMS = pltpu.CompilerParams(vmem_limit_bytes=12 << 20)


def pack_first(keep, events):
    streams, features, length = events.shape
    count = streams * length // LANES
    shapes = [
        pltpu.VMEM((streams, features, 2 * length), F32),
        pltpu.VMEM((count, LANES), F32),
        pltpu.VMEM((count, LANES), I32),
        pltpu.VMEM((count, LANES), I32),
        pltpu.SMEM((8, count), I32),
        pltpu.VMEM((1, features, SPAN), F32),
        pltpu.VMEM((8, LANES), F32),
    ]
    return pl.pallas_call(
        pack_first_body,
        in_specs=[IN_HBM, IN_HBM],
        out_specs=[IN_VMEM] * 4 + [IN_SMEM] + [IN_VMEM] * 2,
        out_shape=shapes,
        scratch_shapes=[
            pltpu.VMEM((streams, length), I32),
            pltpu.VMEM((8, count), I32),
            pltpu.VMEM((2, count, count), BF16),
            pltpu.VMEM((features, length + LANES), F32),
            pltpu.SemaphoreType.DMA,
            pltpu.SemaphoreType.DMA,
            pltpu.SemaphoreType.DMA((streams,)),
        ],
        compiler_params=PARAMS,
        name="pack_first",
    )(
        pltpu.with_memory_space_constraint(keep, pltpu.HBM),
        pltpu.with_memory_space_constraint(events, pltpu.HBM),
    )


def pack(s, length, starts, flat, state, index, slot, number, shared=None):
    streams, features, _ = state.shape
    tiles = length // LANES

    def body(starts, flat, _, index, *refs):
        state, tail, work = refs[-3:]
        pack_stream(s, streams, tiles, flat, state.at[s], index, starts, work, tail.at[slot])

    given = [] if shared is None else [shared]
    return pl.pallas_call(
        body,
        in_specs=[IN_SMEM] + [IN_VMEM] * (3 + len(given)),
        out_specs=[IN_VMEM] * 2,
        out_shape=[
            pltpu.VMEM(state.shape, F32),
            pltpu.VMEM((number, features, SPAN), F32),
        ],
        scratch_shapes=[pltpu.VMEM((features, length + LANES), F32)],
        input_output_aliases={2: 0, **{4 + k: 1 for k in range(len(given))}},
        compiler_params=PARAMS,
        name="pack",
    )(starts, flat, state, index, *given)


def add_totals(length, flat, state, totals):
    streams, features, _ = state.shape
    tiles = length // LANES

    def body(flat, _, so_far, state, totals):
        def step(g, sums):
            sums = list(sums)
            for j in range(GROUP_SUM):
                t = g * GROUP_SUM + j
                at = pl.multiple_of(t * LANES, LANES)
                for s in range(1, streams):
                    kept = state[s, :, pl.ds(at, LANES)] * flat[pl.ds(t * streams + s, 1), :]
                    sums[s - 1] = sums[s - 1] + kept
            return tuple(sums)

        zero = jnp.zeros((features, LANES), F32)
        sums = lax.fori_loop(0, tiles // GROUP_SUM, step, (zero,) * (streams - 1))
        line = jnp.zeros((1, LANES), F32)
        for s in range(1, streams):
            whole_sum = jnp.broadcast_to(
                jnp.sum(sums[s - 1], axis=1, keepdims=True), (features, LANES)
            )
            line = line + totals_line(s, whole_sum)
        sublane = lax.broadcasted_iota(I32, (8, LANES), 0)
        line = jnp.broadcast_to(line, (8, LANES))
        totals[...] = so_far[...] + jnp.where(sublane == 0, line, 0.0)

    return pl.pallas_call(
        body,
        in_specs=[IN_VMEM] * 3,
        out_specs=[IN_VMEM] * 2,
        out_shape=[pltpu.VMEM(state.shape, F32), pltpu.VMEM((8, LANES), F32)],
        input_output_aliases={1: 0},
        compiler_params=PARAMS,
        name="add_totals",
    )(flat, state, totals)


def spread(s, length, starts, arrived, state, ranks, lagging):
    streams, features, _ = state.shape

    def body(starts, arrived, _, ranks, *refs):
        *outs, joint, sent = refs[-4:] if s else (None,) + refs[-3:]
        state = outs[-2] if s else outs[-1]
        write = None
        if s:
            write = pltpu.make_async_copy(means_of(s - 1, length, state), outs[-1].at[s - 1], sent)
            write.start()
        joined(s, length, arrived, state, joint)
        for t in range(length // LANES):
            _, mean = window_mean(s, t, streams, starts, state, ranks, joint)
            state[s, :, length + t * LANES : length + (t + 1) * LANES] = mean
        if write is not None:
            write.wait()

    given = [] if lagging is None else [lagging]
    out_shape = [pltpu.VMEM(state.shape, F32)]
    if s:
        out_shape.append(jax.ShapeDtypeStruct((streams, features, length), F32))
    results = pl.pallas_call(
        body,
        in_specs=[IN_SMEM] + [IN_VMEM] * 3 + [IN_HBM] * len(given),
        out_specs=[IN_VMEM, IN_HBM][: len(out_shape)],
        out_shape=out_shape,
        scratch_shapes=[
            pltpu.VMEM((features, 2 * SPAN + LANES), F32),
            pltpu.SemaphoreType.DMA,
        ],
        input_output_aliases={2: 0, **{4 + k: 1 for k in range(len(given))}},
        compiler_params=PARAMS,
        name="spread",
    )(starts, arrived, state, ranks, *given)
    return (results[0], results[1] if s else None)


def between(chip, brought):
    counts = [len(brought[axis]) for axis in ROWS[:2]]

    def body(chip, *refs):
        *parts, out = refs
        out[...] = jnp.zeros(out.shape, F32)
        out[0:2, :] = chip[0:2, :]
        out[2:4, :] = earlier_rows(parts[: counts[0]], ROWS[0]) + earlier_rows(
            parts[counts[0] :], ROWS[1]
        )

    parts = [part for axis in ROWS[:2] for part in brought[axis]]
    return pl.pallas_call(
        body,
        in_specs=[IN_VMEM] * (1 + len(parts)),
        out_specs=IN_VMEM,
        out_shape=pltpu.VMEM((8, LANES), F32),
        compiler_params=PARAMS,
        name="between",
    )(chip, *parts)


def deviate(length, state, ranks, lagging, own, core, rows, sides):
    streams, features, _ = state.shape
    last = streams - 1
    tiles = length // LANES
    count = ranks.shape[0]

    def body(state, ranks, _, own, *refs):
        core_parts, row_parts = (refs[: len(core)], refs[len(core) : len(refs) - 7])
        at_core = lax.axis_index(ROWS[3])
        row_parts = [
            jnp.where(at_core == sides[k], row_parts[2 * k][0:4, :], row_parts[2 * k + 1][0:4, :])
            for k in range(len(sides))
        ]
        lagging, deviation, columns, scale, staged, sent, gone = refs[-7:]
        writes = [
            pltpu.make_async_copy(means_of(last - 1, length, state), lagging.at[last - 1], sent)
        ]
        writes[0].start()
        before = own[2:4, :] + earlier_rows(core_parts, ROWS[3]) + earlier_rows(row_parts, ROWS[2])
        for part in row_parts:
            before = before + part[2:4, :]
        sums = before[0:1, :]
        row = lax.broadcasted_iota(I32, (features, LANES), 0)
        for s in range(streams):
            chosen = jnp.where(lanes_of(features) == row + s * features, sums, 0.0)
            columns[s] = jnp.broadcast_to(
                jnp.sum(chosen, axis=1, keepdims=True), (features, LANES)
            )
        stream = lax.broadcasted_iota(I32, (count, LANES), 0) & (streams - 1)
        seen = jnp.zeros((count, LANES), F32)
        for s in range(streams):
            tally = jnp.sum(jnp.where(lanes_of(1) == s, before[1:2, :], 0.0))
            seen = jnp.where(stream == s, tally, seen)
        scale[...] = 1.0 / jnp.maximum(seen + ranks[...].astype(F32), 1.0)
        for s in range(last):
            column = columns[s]
            for t in range(tiles):
                at = slice(t * LANES, (t + 1) * LANES)
                mean = state[s, :, length + t * LANES : length + (t + 1) * LANES]
                staged[s, :, at] = mean - (column + state[s, :, at]) * scale[
                    t * streams + s : t * streams + s + 1, :
                ]
            write = pltpu.make_async_copy(staged.at[s], deviation.at[s], gone.at[s])
            write.start()
            writes.append(write)
        for write in writes:
            write.wait()

    shape = jax.ShapeDtypeStruct((streams, features, length), F32)
    return pl.pallas_call(
        body,
        in_specs=[IN_VMEM] * 2 + [IN_HBM] + [IN_VMEM] * (1 + len(core) + len(rows)),
        out_specs=[IN_HBM, IN_HBM, IN_VMEM, IN_VMEM],
        out_shape=[
            shape,
            shape,
            pltpu.VMEM((streams, features, LANES), F32),
            pltpu.VMEM((count, LANES), F32),
        ],
        scratch_shapes=[
            pltpu.VMEM((last, features, length), F32),
            pltpu.SemaphoreType.DMA,
            pltpu.SemaphoreType.DMA((last,)),
        ],
        input_output_aliases={2: 0},
        compiler_params=PARAMS,
        name="deviate",
    )(state, ranks, lagging, own, *core, *rows)


def finish(length, starts, arrived, state, ranks, columns, scale, outputs):
    streams, features, _ = state.shape
    s = streams - 1
    tiles = length // LANES

    def body(starts, arrived, state, ranks, columns, scale, *refs):
        lagging, deviation, joint, means, deviations, sent, gone = refs[-7:]
        joined(s, length, arrived, state, joint)
        column = columns[s]
        writes = []
        for part in range(PARTS):
            for t in range(part * tiles // PARTS, (part + 1) * tiles // PARTS):
                at = slice(t * LANES, (t + 1) * LANES)
                running, mean = window_mean(s, t, streams, starts, state, ranks, joint)
                means[:, at] = mean
                deviations[:, at] = mean - (column + running) * scale[
                    t * streams + s : t * streams + s + 1, :
                ]
            at = pl.ds(part * length // PARTS, length // PARTS)
            for source, target, done in ((means, lagging, sent), (deviations, deviation, gone)):
                writes.append(
                    pltpu.make_async_copy(source.at[:, at], target.at[s, :, at], done.at[part])
                )
                writes[-1].start()
        for write in writes:
            write.wait()

    return pl.pallas_call(
        body,
        in_specs=[IN_SMEM] + [IN_VMEM] * 5 + [IN_HBM] * 2,
        out_specs=[IN_HBM] * 2,
        out_shape=[jax.ShapeDtypeStruct((streams, features, length), F32)] * 2,
        scratch_shapes=[
            pltpu.VMEM((features, 2 * SPAN + LANES), F32),
            pltpu.VMEM((features, length), F32),
            pltpu.VMEM((features, length), F32),
            pltpu.SemaphoreType.DMA((PARTS,)),
            pltpu.SemaphoreType.DMA((PARTS,)),
        ],
        input_output_aliases={6: 0, 7: 1},
        compiler_params=PARAMS,
        name="finish",
    )(starts, arrived, state, ranks, columns, scale, *outputs)


def permuted(value, target):
    places = list(itertools.product(*(range(lax.axis_size(axis)) for axis in ROWS)))
    number = {place: k for k, place in enumerate(places)}
    return lax.ppermute(
        value, ROWS, [(number[place], number[target(*place)]) for place in places]
    )


def exchanged(totals, axis):
    count = lax.axis_size(axis)
    brought = []
    bit = 1
    while bit < count:
        flip = 2 * bit - 1

        def target(z, y, x, core, flip=flip):
            return (z ^ flip, y, x, 1 - core) if axis == ROWS[0] else (z, y ^ flip, x, 1 - core)

        other = permuted(totals, target)
        brought.append(other)
        totals = totals + other
        bit *= 2
    return brought, totals


def other_core(value):
    return permuted(value, lambda z, y, x, core: (z, y, x, 1 - core))


def exchanged_rows(totals):
    count = lax.axis_size(ROWS[2])
    brought, sides = ([], [])
    bit = 1
    while bit < count:
        flip, side = (2 * bit - 1, int(2 * bit >= count))

        def target(z, y, x, core, flip=flip, side=side):
            return (z, y, (x - 1) % count, 1 - side) if core else (z, y, x ^ flip, side)

        other = permuted(totals, target)
        brought += [other, other_core(other)]
        sides.append(side)
        totals = totals + other
        bit *= 2
    return brought, sides


def from_behind(value):
    count = lax.axis_size(ROWS)
    return lax.ppermute(value, ROWS, [(k, (k + 1) % count) for k in range(count)])


def per_device(events, keep):
    streams, _, length = events.shape
    state, flat, index, ranks, starts, tail, totals = pack_first(keep, events)
    arrived = [from_behind(tail)]
    state, totals = add_totals(length, flat, state, totals)
    for s in range(1, streams):
        state, tail = pack(s, length, starts, flat, state, index, 0, 1)
        arrived.append(from_behind(tail))
    brought = {ROWS[3]: [other_core(totals)]}
    chip = totals = totals + brought[ROWS[3]][0]
    for axis in (ROWS[1], ROWS[0]):
        brought[axis], totals = exchanged(totals, axis)
    own = between(chip, brought)
    rows, sides = exchanged_rows(own)
    lagging = None
    for s in range(streams - 1):
        state, lagging = spread(s, length, starts, arrived[s], state, ranks, lagging)
    *outputs, columns, scale = deviate(
        length, state, ranks, lagging, own, brought[ROWS[3]], rows, sides
    )
    return tuple(
        finish(length, starts, arrived[-1], state, ranks, columns, scale, outputs)
    )


def solution(mesh):
    shape = SHAPE if mesh.size == 128 else (1, 1, mesh.size // 2, 2)
    finer = Mesh(mesh.devices.reshape(shape), ROWS)
    in_specs = (P(None, None, ROWS), P(None, ROWS))
    out_specs = (P(None, None, ROWS), P(None, None, ROWS))
    return jax.shard_map(
        per_device, mesh=finer, in_specs=in_specs, out_specs=out_specs, check_vma=False
    )
```
